128 devices in a mesh: seq: 32 (over y, z_hi, x), sub: 4 (over z_lo, core).
Axes of the slice: x: 4, y: 4, z: 4 (z_hi: 2, z_lo: 2; z = z_hi * 2 + z_lo), core: 2. Of those that a mesh axis runs over, the one named last changes fastest.
Arguments:
- tokens: bfloat16 [8192, 4096], P('seq'), may hold values from -6 to 6
- w_split: bfloat16 [4096, 4096], P(None, 'sub'), may hold values from -0.09375 to 0.09375
- w_merge: bfloat16 [4096, 4096], P('sub'), may hold values from -0.09375 to 0.09375
- expert_in: bfloat16 [128, 1024, 2048], P(('seq', 'sub')), may hold values from -0.1875 to 0.1875
- expert_out: bfloat16 [128, 1024, 1024], P(('seq', 'sub')), may hold values from -0.1875 to 0.1875
- expert_ids: int32 [4, 8192, 2], P('sub', 'seq'), may hold values from 0 to 127, all different within a row; in each aligned block of 256 rows (0 to 255, 256 to 511, ..., all dimensions but the last counted through in order) at most 6 rows name the same one
- combine_q: int32 [4, 8192, 2], P('sub', 'seq'), may hold values from 4096 to 65536
- capacity: int32 [128], replicated, may hold values from 3 to 6
Outputs:
- mixed: bfloat16 [8192, 4096], P('seq', 'sub')
The draws below stay inside these ranges and needn't reach their ends.
Inputs may be any that keep to these rules, and one draw needn't show every extreme that they name: `expert_ids`: in each block of 256 positions of one sub-head, the ids of a position differ, no expert is named more than 6 times, a bound that some block reaches.
All inputs are finite; a program needn't handle non-finite values.
Results may differ from the reference program's by a relative error of at most 0.0076.
Values may be sent and summed in bfloat16 or wider, within the bound.
No kernel may reach another device: no remote copies, remote signals or barrier semaphores. Data moves between devices by JAX's collectives and lax.ppermute only.
A program may use at most 128 MiB of HBM per device.

```python
import math
import jax
import jax.numpy as jnp
import numpy as np
from jax import lax

D = 4096
HEADS = 4
FFE = 1024
TOPK = 2
TOK_DEV = 256
SUBW = 1024
EXPERTS = 128
CAP = 6
TOKENS = 8192
N_SEQ = 32


def with_ends(entries, rng, smallest, high):
    longest = entries.shape.index(max(entries.shape))
    spots = []
    for shift in (0, 1):
        where = [jax.random.randint(jax.random.fold_in(rng, axis), (), 0, length) for axis, length in enumerate(entries.shape)]
        where[longest] = (where[longest] + shift) % entries.shape[longest]
        spots.append(tuple(where))
    return entries.at[spots[0]].set(smallest).at[spots[1]].set(high)


def shard_levels(key, extent, split, least, top_value):
    def one(axis_at, blocks):
        draws = jax.random.uniform(jax.random.fold_in(jax.random.fold_in(key, 6), axis_at), (blocks,), jnp.float32, least / len(split), top_value / len(split))
        return jnp.repeat(jnp.exp(draws), extent[axis_at] // blocks).reshape((-1,) + (1,) * (len(extent) - axis_at - 1))

    gain = one(*split[0])
    for cut in split[1:]:
        gain = gain * one(*cut)
    return gain


def deal_out(rng, own, number, rows, number_of, top, limit, lean):
    ranking = jax.random.permutation(rng, number_of)
    crowded, common = shares(number_of, rows * top, limit, lean, True), shares(number_of, rows * top, limit, lean, False)
    places = jnp.arange(number_of)

    def named(lengths, rotation):
        used = int((lengths > 0).sum())
        fixed = max(1, used // 4)
        moved = fixed + (places - fixed + rotation * (used - fixed)) % max(1, number_of - fixed)
        return jnp.zeros((number_of,), jnp.int32).at[ranking[jnp.where(places < fixed, places, moved)]].set(jnp.asarray(lengths, jnp.int32))

    lengths = jnp.where(number % 4 == 0, named(crowded, number // 4), named(common, number - number // 4 - 1))
    mixed = jax.random.permutation(jax.random.fold_in(own, 3), number_of)
    source_of, sink = mixed[0:number_of // 2 * 2:2], mixed[1:number_of // 2 * 2:2]
    slack = jnp.minimum(lengths[source_of] - 1, limit - lengths[sink]) // 2
    slack = jnp.where((source_of == ranking[0]) | (sink == ranking[0]) | (lengths[sink] == 0), 0, jnp.maximum(slack, 0))
    moved = jax.random.randint(jax.random.fold_in(own, 4), (number_of // 2,), 0, 1 << 20) % (slack + 1)
    lengths = lengths.at[source_of].add(-moved).at[sink].add(moved)
    members = jnp.searchsorted(jnp.cumsum(lengths), jnp.arange(rows * top), side="right").astype(jnp.int32)
    table = members.reshape(top, rows).T
    table = table[jax.random.permutation(jax.random.fold_in(own, 1), rows)]
    rotation = jax.random.randint(jax.random.fold_in(own, 2), (rows, 1), 0, top)
    return jnp.take_along_axis(table, (jnp.arange(top)[None, :] + rotation) % top, axis=1)


def shares(number_of, total, limit, slope, full):
    loads = [(1 << 20) // math.isqrt(rank ** slope) + 1 for rank in range(1, number_of + 1)]
    largest = limit if full else min(limit, max(-(-total // number_of), total * loads[0] // sum(loads)))
    least = 1 if total - largest >= number_of - 1 else 0
    counts, rest = [largest] + [least] * (number_of - 1), total - largest - least * (number_of - 1)
    while rest > 0:
        candidates = [i for i in range(1, number_of) if counts[i] < largest] or [i for i in range(1, number_of) if counts[i] < limit]
        mass, remaining = sum([loads[i] for i in candidates]), rest
        for i in candidates:
            addition = min(limit - counts[i], max(1, remaining * loads[i] // mass), rest)
            counts[i] = counts[i] + addition
            rest = rest - addition
    return np.array(counts)


def centred(key, shape, scale, bound, split=(), kind=jnp.bfloat16):
    array = scale * jax.random.normal(key, shape, jnp.float32)
    if split:
        array = array * shard_levels(key, shape, split, -0.22, 0.18)
    return jnp.clip(array, -bound, bound).astype(kind)


def setup_inputs(seed: int = 0) -> dict:
    key_of = jax.random.split(jax.random.key(seed), 9)
    tokens = centred(key_of[0], (TOKENS, D), 1.0, 6.0, ((0, 32),))
    w_split = centred(key_of[1], (D, D), D ** -0.5, 0.09375, ((1, 4),))
    w_merge = centred(key_of[2], (D, D), D ** -0.5, 0.09375, ((0, 4),))
    expert_in = centred(key_of[3], (EXPERTS, SUBW, 2 * FFE), SUBW ** -0.5, 0.1875, ((0, 128),))
    expert_out = centred(key_of[4], (EXPERTS, FFE, SUBW), FFE ** -0.5, 0.1875, ((0, 128),))
    expert_ids_keys = jax.random.split(jax.random.fold_in(key_of[5], 1), HEADS * TOKENS // TOK_DEV)
    expert_ids_turns = jax.random.permutation(jax.random.fold_in(key_of[5], 3), HEADS * TOKENS // TOK_DEV)
    expert_ids = jax.vmap(lambda own, number: deal_out(jax.random.fold_in(key_of[5], 2), own, number, TOK_DEV, EXPERTS, TOPK, CAP, 2))(expert_ids_keys, expert_ids_turns).reshape((HEADS, TOKENS, TOPK))
    combine_q = with_ends(jax.random.randint(key_of[6], (HEADS, TOKENS, TOPK), 4096, 65537), jax.random.fold_in(key_of[6], 1), 4096, 65536).astype(jnp.int32)
    capacity = with_ends(jax.random.randint(key_of[7], (EXPERTS,), CAP // 2, CAP + 1), jax.random.fold_in(key_of[7], 1), CAP // 2, CAP).astype(jnp.int32)
    return {"tokens": tokens, "w_split": w_split, "w_merge": w_merge, "expert_in": expert_in, "expert_out": expert_out, "expert_ids": expert_ids, "combine_q": combine_q, "capacity": capacity}


def expert_ffn(inputs, w_in, w_out):
    gate_up = jnp.dot(inputs, w_in, preferred_element_type=jnp.float32)
    ffe_width = w_out.shape[0]
    hidden = (jax.nn.silu(gate_up[:, :ffe_width]) * gate_up[:, ffe_width:]).astype(jnp.bfloat16)
    return jnp.dot(hidden, w_out, preferred_element_type=jnp.float32).astype(jnp.bfloat16)


def reference(tokens, w_split, w_merge, expert_in, expert_out, expert_ids, combine_q, capacity):
    sub_tokens = jnp.dot(tokens, w_split, preferred_element_type=jnp.float32).astype(jnp.bfloat16)
    table = sub_tokens.reshape(TOKENS, HEADS, SUBW).transpose(1, 0, 2).reshape(HEADS * TOKENS, SUBW)
    block_count = HEADS * N_SEQ
    expert_of = expert_ids.reshape(block_count, TOPK * TOK_DEV)
    onehot = (expert_of[:, :, None] == jnp.arange(EXPERTS, dtype=jnp.int32)[None, None, :]).astype(jnp.int32)
    order_rank = jnp.sum((jnp.cumsum(onehot, axis=1) - onehot) * onehot, axis=2)
    cap_limit = jnp.sum(onehot * capacity[None, None, :], axis=2)
    is_kept = order_rank < cap_limit
    block_id = jnp.arange(block_count, dtype=jnp.int32)[:, None]
    slot_index = (expert_of * block_count + block_id) * CAP + order_rank
    total_slots = EXPERTS * block_count * CAP
    slot_index = jnp.where(is_kept, slot_index, total_slots)
    entry_pos = jnp.arange(TOPK * TOK_DEV, dtype=jnp.int32)[None, :]
    row_index = block_id * TOK_DEV + entry_pos // TOPK
    weights = combine_q.reshape(block_count, TOPK * TOK_DEV).astype(jnp.float32) / 65536.0
    slot_row = jnp.full((total_slots,), -1, jnp.int32).at[slot_index.reshape(-1)].set(
        jnp.broadcast_to(row_index, slot_index.shape).reshape(-1), mode="drop")
    slot_weight = jnp.zeros((total_slots,), jnp.float32).at[slot_index.reshape(-1)].set(
        weights.reshape(-1), mode="drop")
    slot_row = slot_row.reshape(EXPERTS, block_count * CAP)
    slot_weight = slot_weight.reshape(EXPERTS, block_count * CAP)

    def one_expert(running, inputs_e):
        rows_here, weights_here, w_in, w_out = inputs_e
        is_valid = rows_here >= 0
        safe_row = jnp.maximum(rows_here, 0)
        picked = jnp.where(is_valid[:, None], table[safe_row], jnp.zeros((), jnp.bfloat16))
        answer = expert_ffn(picked, w_in, w_out)
        weighted = jnp.where(is_valid[:, None], weights_here[:, None] * answer.astype(jnp.float32), jnp.zeros((), jnp.float32))
        return running.at[safe_row].add(weighted), None

    start = jnp.zeros((HEADS * TOKENS, SUBW), jnp.float32)
    running, _ = lax.scan(one_expert, start, (slot_row, slot_weight, expert_in, expert_out))
    head_out = running.astype(jnp.bfloat16).reshape(HEADS, TOKENS, SUBW).transpose(1, 0, 2).reshape(TOKENS, D)
    return jnp.dot(head_out, w_merge, preferred_element_type=jnp.float32).astype(jnp.bfloat16)
```

```python
import jax
import jax.numpy as jnp
from jax import lax
from jax.experimental import pallas as pl
from jax.experimental.pallas import tpu as pltpu
from jax.sharding import PartitionSpec as P

F32 = jnp.float32
BF16 = jnp.bfloat16
I32 = jnp.int32

SLOTS = 6
ROWS = 8
WIDE = 768
LANES = 256
TAILS = 3
NONE = -4.0


def iota(shape, dim):
    return lax.broadcasted_iota(I32, shape, dim)


def dot(a, b):
    return jnp.dot(a, b, preferred_element_type=F32)


def slot_of_row(row, part):
    if part is None:
        return jnp.where(row < SLOTS, row, -2)
    return jnp.where(row < SLOTS, -2, part + TAILS * (row - SLOTS))


def slot_keys(ids, capacity):
    experts = capacity.shape[1]
    tokens = ids.shape[1]
    expert = iota((experts, tokens), 0)
    named = (ids[0:1, :] == expert) | (ids[1:2, :] == expert)
    earlier = (iota((tokens, tokens), 0) < iota((tokens, tokens), 1)).astype(F32).astype(BF16)
    rank = dot(named.astype(F32).astype(BF16), earlier)
    own = iota((experts, experts), 0) == iota((experts, experts), 1)
    limit = jnp.sum(jnp.where(own, capacity.astype(F32), 0.0), axis=1, keepdims=True)
    return jnp.where(named & (rank < limit), rank, NONE)


def pack_body(ids_ref, cap_ref, tok_ref, w_ref, out_ref, acc_ref, pick_ref):
    step = pl.program_id(0)
    rows = out_ref.shape[0]

    @pl.when(step == 0)
    def _():
        key = slot_keys(ids_ref[...], cap_ref[...])
        experts = key.shape[0]
        spread = ((iota((rows, experts), 0) >> 3) == iota((rows, experts), 1)).astype(F32).astype(BF16)
        key = dot(spread, key.astype(BF16))
        row = iota(key.shape, 0) & (ROWS - 1)
        for n, part in enumerate((None, 0, 1, 2)):
            pick_ref[n] = (key == slot_of_row(row, part).astype(F32)).astype(F32).astype(BF16)
        acc_ref[...] = dot(tok_ref[...], w_ref[...])

    @pl.when(step > 0)
    def _():
        acc_ref[...] += dot(tok_ref[...], w_ref[...])

    @pl.when(step == pl.num_programs(0) - 1)
    def _():
        sub = acc_ref[...].astype(BF16)
        tail = sub[:, WIDE:]
        for k in range(TAILS):
            cols = slice(k * LANES, (k + 1) * LANES)
            packed = dot(pick_ref[0], sub[:, cols]) + dot(pick_ref[k + 1], tail)
            out_ref[:, cols] = packed.astype(BF16)


def split_and_pack(ids, capacity, tokens, w_split, steps=4):
    count, depth = tokens.shape
    width = w_split.shape[1]
    rows = capacity.shape[1] * ROWS
    part = depth // steps
    return pl.pallas_call(
        pack_body,
        grid=(steps,),
        in_specs=[
            pl.BlockSpec(ids.shape, lambda i: (0, 0)),
            pl.BlockSpec(capacity.shape, lambda i: (0, 0)),
            pl.BlockSpec((count, part), lambda i: (0, i)),
            pl.BlockSpec((part, width), lambda i: (i, 0)),
        ],
        out_specs=pl.BlockSpec((rows, WIDE), lambda i: (0, 0)),
        out_shape=jax.ShapeDtypeStruct((rows, WIDE), BF16),
        scratch_shapes=[pltpu.VMEM((count, width), F32), pltpu.VMEM((4, rows, count), BF16)],
        compiler_params=pltpu.CompilerParams(vmem_limit_bytes=24 << 20),
        name="split_pack",
    )(ids, capacity, tokens, w_split)


def weights_body(ids_ref, cap_ref, q_ref, out_ref):
    ids = ids_ref[...]
    key = slot_keys(ids, cap_ref[...])
    experts, tokens = key.shape
    expert = iota((experts, tokens), 0)
    scale = q_ref[...].astype(F32) / 65536.0
    weight = jnp.where(ids[0:1, :] == expert, scale[0:1, :], 0.0) + jnp.where(ids[1:2, :] == expert, scale[1:2, :], 0.0)
    cols = out_ref.shape[2]
    spread = ((iota((experts, cols), 1) >> 3) == iota((experts, cols), 0)).astype(F32).astype(BF16)
    key = dot(key.T.astype(BF16), spread)
    weight = dot(weight.T.astype(BF16), spread)
    row = iota(key.shape, 1) & (ROWS - 1)
    for n, part in enumerate((None, 0, 1, 2)):
        out_ref[n] = jnp.where(key == slot_of_row(row, part).astype(F32), weight, 0.0).astype(BF16)


def combine_weights(ids, capacity, q):
    tokens = ids.shape[1]
    cols = capacity.shape[1] * ROWS
    return pl.pallas_call(
        weights_body,
        out_shape=jax.ShapeDtypeStruct((4, tokens, cols), BF16),
        compiler_params=pltpu.CompilerParams(vmem_limit_bytes=24 << 20),
        name="combine_weights",
    )(ids, capacity, q)


GROUP = 16


def sixth(x):
    return (x * 43) >> 8


def unpack_picks():
    shape = (GROUP * SLOTS, GROUP * ROWS)
    to, frm = iota(shape, 0), iota(shape, 1)
    slot = to - sixth(to) * SLOTS
    same = sixth(to) == (frm >> 3)
    row = frm & (ROWS - 1)
    return [(same & (slot_of_row(row, part) == slot)).astype(F32).astype(BF16) for part in (None, 0, 1, 2)]


def pack_picks():
    shape = (GROUP * ROWS, GROUP * SLOTS)
    frm, to = iota(shape, 1), iota(shape, 0)
    slot = frm - sixth(frm) * SLOTS
    same = sixth(frm) == (to >> 3)
    row = to & (ROWS - 1)
    return [(same & (slot_of_row(row, part) == slot)).astype(F32).astype(BF16) for part in (None, 0, 1, 2)]


def expert_body(x_ref, gate_ref, up_ref, down_ref, out_ref, rows_ref, act_ref, tail_ref):
    step = pl.program_id(0)
    half = pl.num_programs(0) // 2
    groups = x_ref.shape[0] // (GROUP * ROWS)

    @pl.when(step == 0)
    def _():
        picks = unpack_picks()
        for g in range(groups):
            tiles = x_ref[g * GROUP * ROWS : (g + 1) * GROUP * ROWS, :]
            into = slice(g * GROUP * SLOTS, (g + 1) * GROUP * SLOTS)
            rows_ref[into, :WIDE] = dot(picks[0], tiles).astype(BF16)
            tail = dot(picks[1], tiles[:, :LANES])
            for k in range(1, TAILS):
                tail += dot(picks[k + 1], tiles[:, k * LANES : (k + 1) * LANES])
            rows_ref[into, WIDE:] = tail.astype(BF16)

    for j in range(4):

        @pl.when(step == j)
        def _():
            rows = rows_ref[...]
            gate = dot(rows, gate_ref[0])
            up = dot(rows, up_ref[0])
            act_ref[:, j * LANES : (j + 1) * LANES] = (gate / (1.0 + jnp.exp(-gate)) * up).astype(BF16)

    @pl.when(step == half)
    def _():
        tail_ref[...] = dot(act_ref[...], down_ref[0]).astype(BF16)

    for k in range(TAILS):

        @pl.when(step == half + 1 + k)
        def _():
            answer = dot(act_ref[...], down_ref[0]).astype(BF16)
            picks = pack_picks()
            for g in range(groups):
                frm = slice(g * GROUP * SLOTS, (g + 1) * GROUP * SLOTS)
                packed = dot(picks[0], answer[frm, :]) + dot(picks[k + 1], tail_ref[frm, :])
                out_ref[g * GROUP * ROWS : (g + 1) * GROUP * ROWS, k * LANES : (k + 1) * LANES] = packed.astype(BF16)


def expert_rows(tiles, expert_in, expert_out):
    rows = tiles.shape[0]
    slots = rows // ROWS * SLOTS
    width = expert_in.shape[1]
    hidden = expert_out.shape[1]
    return pl.pallas_call(
        expert_body,
        grid=(8,),
        in_specs=[
            pl.BlockSpec((rows, WIDE), lambda i: (0, 0)),
            pl.BlockSpec((1, width, LANES), lambda i: (0, 0, jnp.minimum(i, 3))),
            pl.BlockSpec((1, width, LANES), lambda i: (0, 0, 4 + jnp.minimum(i, 3))),
            pl.BlockSpec((1, hidden, LANES), lambda i: (0, 0, jnp.where(i < 5, 3, i - 5))),
        ],
        out_specs=pl.BlockSpec((rows, WIDE), lambda i: (0, 0)),
        out_shape=jax.ShapeDtypeStruct((rows, WIDE), BF16),
        scratch_shapes=[
            pltpu.VMEM((slots, width), BF16),
            pltpu.VMEM((slots, hidden), BF16),
            pltpu.VMEM((slots, LANES), BF16),
        ],
        compiler_params=pltpu.CompilerParams(vmem_limit_bytes=32 << 20),
        name="experts",
    )(tiles, expert_in, expert_in, expert_out)


def combine_body(at_ref, v_ref, b_ref, w_ref, head_ref, send_ref, keep_ref):
    step = pl.program_id(0)
    del at_ref

    @pl.when(step == 0)
    def _():
        tail = jnp.zeros((head_ref.shape[0], LANES), F32)
        for k in range(TAILS):
            cols = slice(k * LANES, (k + 1) * LANES)
            back = b_ref[:, cols]
            head_ref[:, cols] = dot(v_ref[0], back).astype(BF16)
            tail += dot(v_ref[k + 1], back)
        head_ref[:, WIDE:] = tail.astype(BF16)

    part = dot(head_ref[...], w_ref[...]).astype(BF16)
    width = part.shape[1]
    for j in range(2):

        @pl.when(step == j)
        def _():
            send_ref[:, j * width : (j + 1) * width] = part

        @pl.when(step == 2 + j)
        def _():
            keep_ref[:, j * width : (j + 1) * width] = part


def combine_and_merge(at, v, back, w_merge):
    tokens = v.shape[1]
    width = w_merge.shape[0]
    whole = lambda i, at: (0, 0)
    return pl.pallas_call(
        combine_body,
        grid_spec=pltpu.PrefetchScalarGridSpec(
            num_scalar_prefetch=1,
            grid=(4,),
            in_specs=[
                pl.BlockSpec(v.shape, lambda i, at: (0, 0, 0)),
                pl.BlockSpec(back.shape, whole),
                pl.BlockSpec((width, width // 2), lambda i, at: (0, at[i // 2] * 2 + i % 2)),
            ],
            out_specs=[pl.BlockSpec((tokens, width), whole)] * 3,
        ),
        out_shape=[jax.ShapeDtypeStruct((tokens, width), BF16)] * 3,
        compiler_params=pltpu.CompilerParams(vmem_limit_bytes=32 << 20),
        name="combine_merge",
    )(at, v, back, w_merge)


def merge_body(at_ref, head_ref, w_ref, send_ref, keep_ref):
    step = pl.program_id(0)
    del at_ref
    part = dot(head_ref[...], w_ref[...]).astype(BF16)
    width = part.shape[1]
    for j in range(2):

        @pl.when(step == j)
        def _():
            send_ref[:, j * width : (j + 1) * width] = part

        @pl.when(step == 2 + j)
        def _():
            keep_ref[:, j * width : (j + 1) * width] = part


def merge_own(at, head, w_merge):
    tokens, width = head.shape
    whole = lambda i, at: (0, 0)
    return pl.pallas_call(
        merge_body,
        grid_spec=pltpu.PrefetchScalarGridSpec(
            num_scalar_prefetch=1,
            grid=(4,),
            in_specs=[
                pl.BlockSpec(head.shape, whole),
                pl.BlockSpec((width, width // 2), lambda i, at: (0, at[i // 2] * 2 + i % 2)),
            ],
            out_specs=[pl.BlockSpec((tokens, width), whole)] * 2,
        ),
        out_shape=[jax.ShapeDtypeStruct((tokens, width), BF16)] * 2,
        compiler_params=pltpu.CompilerParams(vmem_limit_bytes=32 << 20),
        name="merge_own",
    )(at, head, w_merge)


def exchange(tiles, axes):
    peers = tiles.shape[0] // ROWS
    return lax.all_to_all(tiles.reshape(peers, ROWS, WIDE), axes, split_axis=0, concat_axis=0, tiled=True).reshape(tiles.shape)


def added(a, b):
    return (a.astype(F32) + b.astype(F32)).astype(BF16)


def body(tokens, w_split, w_merge, expert_in, expert_out, expert_ids, combine_q, capacity):
    ids = expert_ids[0].T
    q = combine_q[0].T
    limit = capacity.reshape(1, -1)
    tiles = exchange(split_and_pack(ids, limit, tokens, w_split), ("seq", "sub"))
    v = combine_weights(ids, limit, q)
    back = exchange(expert_rows(tiles, expert_in, expert_out), ("seq", "sub"))

    me = lax.axis_index("sub")
    core = [(i, i ^ 1) for i in range(4)]
    chip = [(i, i ^ 2) for i in range(4)]
    head, far_send, far_keep = combine_and_merge(jnp.stack([me ^ 3, me ^ 2]), v, back, w_merge)
    far_in = lax.ppermute(far_send, "sub", core)
    own_send, own_keep = merge_own(jnp.stack([me ^ 1, me]), head, w_merge)
    cross = lax.ppermute(added(far_keep, far_in), "sub", chip)
    own_in = lax.ppermute(own_send, "sub", core)
    return (own_keep.astype(F32) + own_in.astype(F32) + cross.astype(F32)).astype(BF16)


def solution(mesh):
    in_specs = (
        P("seq", None),
        P(None, "sub"),
        P("sub", None),
        P(("seq", "sub"), None, None),
        P(("seq", "sub"), None, None),
        P("sub", "seq", None),
        P("sub", "seq", None),
        P(),
    )
    out_specs = P("seq", "sub")
    return jax.shard_map(body, mesh=mesh, in_specs=in_specs, out_specs=out_specs, check_vma=False)
```

```python
import jax
import jax.numpy as jnp
from jax import lax
from jax.experimental import pallas as pl
from jax.experimental.pallas import tpu as pltpu
from jax.sharding import PartitionSpec as P

F32 = jnp.float32
BF16 = jnp.bfloat16
I32 = jnp.int32

SLOTS = 6
CHUNKS = 2
EACH = SLOTS // CHUNKS
ROWS = 8
WIDTH = 1024
LANES = EACH * WIDTH // ROWS
NONE = -4.0
FULL = 60 * 1024 * 1024


def pieces(slot):
    whole = WIDTH // LANES
    out = [(j * EACH + slot, 0, j * LANES, LANES) for j in range(whole)]
    rest = WIDTH - whole * LANES
    if rest:
        free = ROWS - whole * EACH
        each = LANES // EACH if free * LANES // EACH == rest and EACH == 3 else rest
        if EACH == 3:
            out += [(whole * EACH + j, slot * each, whole * LANES + j * each, each) for j in range(free)]
        else:
            out += [(whole * EACH + slot // 3, (slot % 3) * rest, whole * LANES, rest)]
    return out


def iota(shape, dim):
    return lax.broadcasted_iota(I32, shape, dim)


def dot(a, b):
    return jnp.dot(a, b, preferred_element_type=F32)


def bits(mask):
    return mask.astype(F32).astype(BF16)


def to_tiles(out_ref, flat_ref, values):
    peers = values.shape[0] // EACH
    for s in range(EACH):
        for row, lane, col, width in pieces(s):
            for w in range(0, width, 128):
                flat_ref[(lane + w) // 128, pl.ds(row, peers, stride=ROWS), :] = values[
                    s * peers : (s + 1) * peers, col + w : col + w + 128
                ]
    for b in range(LANES // 128):
        out_ref[:, b * 128 : (b + 1) * 128] = flat_ref[b].astype(BF16)


def from_tiles(rows_ref, flat_ref, in_ref):
    peers = in_ref.shape[0] // ROWS
    for b in range(LANES // 128):
        flat_ref[b] = in_ref[:, b * 128 : (b + 1) * 128].astype(F32)
    for s in range(EACH):
        for row, lane, col, width in pieces(s):
            for w in range(0, width, 128):
                rows_ref[s * peers : (s + 1) * peers, col + w : col + w + 128] = flat_ref[
                    (lane + w) // 128, pl.ds(row, peers, stride=ROWS), :
                ].astype(BF16)


def slot_keys(ids, capacity):
    experts = capacity.shape[1]
    tokens = ids.shape[1]
    expert = iota((experts, tokens), 0)
    named = (ids[0:1, :] == expert) | (ids[1:2, :] == expert)
    earlier = bits(iota((tokens, tokens), 0) < iota((tokens, tokens), 1))
    rank = dot(bits(named), earlier)
    own = iota((experts, experts), 0) == iota((experts, experts), 1)
    limit = jnp.sum(jnp.where(own, capacity.astype(F32), 0.0), axis=1, keepdims=True)
    return jnp.where(named & (rank < limit), rank, NONE)


def pack_body(ids_ref, cap_ref, tok_ref, w_ref, *refs):
    out_refs, (acc_ref, pick_ref, flat_ref) = refs[:CHUNKS], refs[CHUNKS:]
    step = pl.program_id(0)

    @pl.when(step == 0)
    def _():
        key = slot_keys(ids_ref[...], cap_ref[...])
        peers = key.shape[0]
        for s in range(SLOTS):
            pick_ref[s * peers : (s + 1) * peers, :] = bits(key == float(s))
        acc_ref[...] = dot(tok_ref[...], w_ref[...])

    @pl.when(step > 0)
    def _():
        acc_ref[...] += dot(tok_ref[...], w_ref[...])

    @pl.when(step == pl.num_programs(0) - 1)
    def _():
        sub = acc_ref[...].astype(BF16)
        rows = pick_ref.shape[0] // CHUNKS
        for c in range(CHUNKS):
            to_tiles(out_refs[c], flat_ref, dot(pick_ref[c * rows : (c + 1) * rows, :], sub))


def flat_scratch(rows):
    return pltpu.VMEM((LANES // 128, rows, 128), F32)


def split_and_pack(ids, capacity, tokens, w_split, steps=4):
    count, depth = tokens.shape
    width = w_split.shape[1]
    experts = capacity.shape[1]
    rows = experts * ROWS
    part = depth // steps
    return pl.pallas_call(
        pack_body,
        grid=(steps,),
        in_specs=[
            pl.BlockSpec(ids.shape, lambda i: (0, 0)),
            pl.BlockSpec(capacity.shape, lambda i: (0, 0)),
            pl.BlockSpec((count, part), lambda i: (0, i)),
            pl.BlockSpec((part, width), lambda i: (i, 0)),
        ],
        out_specs=[pl.BlockSpec((rows, LANES), lambda i: (0, 0))] * CHUNKS,
        out_shape=[jax.ShapeDtypeStruct((rows, LANES), BF16)] * CHUNKS,
        scratch_shapes=[pltpu.VMEM((count, width), F32), pltpu.VMEM((experts * SLOTS, count), BF16), flat_scratch(rows)],
        compiler_params=pltpu.CompilerParams(vmem_limit_bytes=FULL),
        name="split_pack",
    )(ids, capacity, tokens, w_split)


def weights_body(ids_ref, cap_ref, q_ref, out_ref):
    ids = ids_ref[...]
    key = slot_keys(ids, cap_ref[...])
    expert = iota(key.shape, 0)
    scale = q_ref[...].astype(F32) / 65536.0
    weight = jnp.where(ids[0:1, :] == expert, scale[0:1, :], 0.0) + jnp.where(ids[1:2, :] == expert, scale[1:2, :], 0.0)
    key, weight = key.T, weight.T
    peers = key.shape[1]
    for s in range(SLOTS):
        out_ref[:, s * peers : (s + 1) * peers] = jnp.where(key == float(s), weight, 0.0).astype(BF16)


def combine_weights(ids, capacity, q):
    return pl.pallas_call(
        weights_body,
        out_shape=jax.ShapeDtypeStruct((ids.shape[1], capacity.shape[1] * SLOTS), BF16),
        compiler_params=pltpu.CompilerParams(vmem_limit_bytes=FULL),
        name="combine_weights",
    )(ids, capacity, q)


def fetch(copies):
    for c in copies:
        c.start()
    return copies


def expert_body(x_hbm, in_hbm, down_hbm, out_ref, x_ref, in_ref, down_ref, rows_ref, act_ref, flat_ref, sems):
    hidden = down_ref.shape[0]
    part = hidden // 4
    copy = pltpu.make_async_copy
    get_x = fetch([copy(x_hbm, x_ref, sems.at[0])])[0]
    get_in = []
    for j in range(4):
        for n, col in enumerate((j * part, hidden + j * part)):
            cols = pl.ds(col, part)
            get_in.append(copy(in_hbm.at[0, :, cols], in_ref.at[:, cols], sems.at[1 + 2 * j + n]))
    fetch(get_in)
    get_down = fetch([copy(down_hbm.at[0], down_ref, sems.at[9])])[0]
    get_x.wait()
    from_tiles(rows_ref, flat_ref, x_ref)
    rows = rows_ref[...]
    for j in range(4):
        get_in[2 * j].wait()
        get_in[2 * j + 1].wait()
        gate = dot(rows, in_ref[:, j * part : (j + 1) * part])
        up = dot(rows, in_ref[:, hidden + j * part : hidden + (j + 1) * part])
        act_ref[:, j * part : (j + 1) * part] = (gate / (1.0 + jnp.exp(-gate)) * up).astype(BF16)
    get_down.wait()
    to_tiles(out_ref, flat_ref, dot(act_ref[...], down_ref[...]))


def expert_rows(tiles, expert_in, expert_out):
    rows = tiles.shape[0]
    slots = rows // ROWS * EACH
    width = expert_in.shape[1]
    hidden = expert_out.shape[1]
    return pl.pallas_call(
        expert_body,
        out_shape=jax.ShapeDtypeStruct((rows, LANES), BF16),
        in_specs=[pl.BlockSpec(memory_space=pltpu.HBM)] * 3,
        scratch_shapes=[
            pltpu.VMEM((rows, LANES), BF16),
            pltpu.VMEM((width, 2 * hidden), BF16),
            pltpu.VMEM((hidden, width), BF16),
            pltpu.VMEM((slots, width), BF16),
            pltpu.VMEM((slots, hidden), BF16),
            flat_scratch(rows),
            pltpu.SemaphoreType.DMA((10,)),
        ],
        compiler_params=pltpu.CompilerParams(vmem_limit_bytes=FULL),
        name="experts",
    )(tiles, expert_in, expert_out)


def part_body(v_ref, b_ref, out_ref, rows_ref, flat_ref):
    from_tiles(rows_ref, flat_ref, b_ref)
    out_ref[...] = dot(v_ref[...], rows_ref[...])


def combine_part(v, back):
    rows = back.shape[0]
    return pl.pallas_call(
        part_body,
        grid=(1,),
        in_specs=[
            pl.BlockSpec((v.shape[0], v.shape[1] // CHUNKS), lambda i: (0, 0)),
            pl.BlockSpec(back.shape, lambda i: (0, 0)),
        ],
        out_specs=pl.BlockSpec((v.shape[0], WIDTH), lambda i: (0, 0)),
        out_shape=jax.ShapeDtypeStruct((v.shape[0], WIDTH), F32),
        scratch_shapes=[pltpu.VMEM((rows // ROWS * EACH, WIDTH), BF16), flat_scratch(rows)],
        compiler_params=pltpu.CompilerParams(vmem_limit_bytes=FULL),
        name="combine_part",
    )(v, back)


def column_block(w_hbm, at, width):
    return w_hbm.at[:, pl.ds(pl.multiple_of(at * width, width), width)]


def combine_body(at_ref, v_hbm, b_hbm, *refs):
    part_hbm, refs = refs[: CHUNKS - 1], refs[CHUNKS - 1 :]
    w_hbm, head_ref, send_ref, v_ref, b_ref, part_ref, w_ref, rows_ref, flat_ref, sems = refs
    width = w_ref.shape[0]
    copy = pltpu.make_async_copy
    get_b = copy(b_hbm, b_ref, sems.at[0])
    get_v = copy(v_hbm.at[:, pl.ds((CHUNKS - 1) * v_ref.shape[1], v_ref.shape[1])], v_ref, sems.at[1])
    get_w = copy(column_block(w_hbm, at_ref[0], width), w_ref, sems.at[2])
    get_part = [copy(p, part_ref.at[n], sems.at[3 + n]) for n, p in enumerate(part_hbm)]
    fetch([get_b, get_v, get_w] + get_part)
    get_b.wait()
    from_tiles(rows_ref, flat_ref, b_ref)
    get_v.wait()
    head = dot(v_ref[...], rows_ref[...])
    for n, get in enumerate(get_part):
        get.wait()
        head += part_ref[n]
    head = head.astype(BF16)
    head_ref[...] = head
    get_w.wait()
    send_ref[...] = dot(head, w_ref[...]).astype(BF16)


def combine_and_merge(at, v, back, part, w_merge):
    tokens = v.shape[0]
    width = w_merge.shape[0]
    rows = back.shape[0]
    return pl.pallas_call(
        combine_body,
        in_specs=[pl.BlockSpec(memory_space=pltpu.SMEM)] + [pl.BlockSpec(memory_space=pltpu.HBM)] * (CHUNKS + 2),
        out_shape=[jax.ShapeDtypeStruct((tokens, width), BF16)] * 2,
        scratch_shapes=[
            pltpu.VMEM((tokens, v.shape[1] // CHUNKS), BF16),
            pltpu.VMEM(back.shape, BF16),
            pltpu.VMEM((max(CHUNKS - 1, 1), tokens, width), F32),
            pltpu.VMEM((width, width), BF16),
            pltpu.VMEM((rows // ROWS * EACH, width), BF16),
            flat_scratch(rows),
            pltpu.SemaphoreType.DMA((3 + CHUNKS,)),
        ],
        compiler_params=pltpu.CompilerParams(vmem_limit_bytes=FULL),
        name="combine_merge",
    )(at, v, back, *part, w_merge)


def merge_body(at_ref, head_ref, w_hbm, far_ref, send_ref, keep_ref, w_ref, sems):
    width = w_ref.shape[1]
    gets = [
        pltpu.make_async_copy(column_block(w_hbm, at_ref[1 + n], width), w_ref.at[n], sems.at[n]) for n in range(3)
    ]
    fetch(gets)
    head = head_ref[...]
    for n, out_ref in enumerate((far_ref, send_ref, keep_ref)):
        gets[n].wait()
        out_ref[...] = dot(head, w_ref[n]).astype(BF16)


def merge_rest(at, head, w_merge):
    tokens, width = head.shape
    whole = pl.BlockSpec((tokens, width), lambda: (0, 0))
    return pl.pallas_call(
        merge_body,
        in_specs=[pl.BlockSpec(memory_space=pltpu.SMEM), whole, pl.BlockSpec(memory_space=pltpu.HBM)],
        out_specs=[whole] * 3,
        out_shape=[jax.ShapeDtypeStruct((tokens, width), BF16)] * 3,
        scratch_shapes=[pltpu.VMEM((3, width, width), BF16), pltpu.SemaphoreType.DMA((3,))],
        compiler_params=pltpu.CompilerParams(vmem_limit_bytes=FULL),
        name="merge_rest",
    )(at, head, w_merge)


def exchange(tiles, axes):
    peers = tiles.shape[0] // ROWS
    return lax.all_to_all(tiles.reshape(peers, ROWS, LANES), axes, split_axis=0, concat_axis=0, tiled=True).reshape(tiles.shape)


def added(a, b):
    return (a.astype(F32) + b.astype(F32)).astype(BF16)


def body(tokens, w_split, w_merge, expert_in, expert_out, expert_ids, combine_q, capacity):
    ids = expert_ids[0].T
    q = combine_q[0].T
    limit = capacity.reshape(1, -1)
    axes = ("seq", "sub")
    tiles = [exchange(t, axes) for t in split_and_pack(ids, limit, tokens, w_split)]
    v = combine_weights(ids, limit, q)
    back = [exchange(expert_rows(t, expert_in, expert_out), axes) for t in tiles]

    me = lax.axis_index("sub")
    core = [(i, i ^ 1) for i in range(4)]
    chip = [(i, i ^ 2) for i in range(4)]
    at = me ^ jnp.array([3, 2, 1, 0], I32)
    part = [combine_part(v, b) for b in back[:-1]]
    head, far_send = combine_and_merge(at, v, back[-1], part, w_merge)
    far_in = lax.ppermute(far_send, "sub", core)
    far_keep, own_send, own_keep = merge_rest(at, head, w_merge)
    cross = lax.ppermute(added(far_keep, far_in), "sub", chip)
    own_in = lax.ppermute(own_send, "sub", core)
    return (own_keep.astype(F32) + own_in.astype(F32) + cross.astype(F32)).astype(BF16)


def solution(mesh):
    in_specs = (
        P("seq", None),
        P(None, "sub"),
        P("sub", None),
        P(("seq", "sub"), None, None),
        P(("seq", "sub"), None, None),
        P("sub", "seq", None),
        P("sub", "seq", None),
        P(),
    )
    out_specs = P("seq", "sub")
    return jax.shard_map(body, mesh=mesh, in_specs=in_specs, out_specs=out_specs, check_vma=False)
```

```python
import jax
import jax.numpy as jnp
from jax import lax
from jax.experimental import pallas as pl
from jax.experimental.pallas import tpu as pltpu
from jax.sharding import PartitionSpec as P

F32 = jnp.float32
BF16 = jnp.bfloat16
I32 = jnp.int32

SLOTS = 6
ROWS = 8
WIDTH = 1024
LANES = SLOTS * WIDTH // ROWS
NONE = -4.0


def pieces(slot):
    rest = WIDTH - LANES
    return [(slot, 0, 0, LANES), (SLOTS + slot // 3, slot % 3 * rest, LANES, rest)]


def iota(shape, dim):
    return lax.broadcasted_iota(I32, shape, dim)


def dot(a, b):
    return jnp.dot(a, b, preferred_element_type=F32)


def bits(mask):
    return mask.astype(F32).astype(BF16)


def to_flat(flat_ref, values, first=0):
    peers = values.shape[0] // SLOTS
    last = first + values.shape[1]
    for s in range(SLOTS):
        for row, lane, col, width in pieces(s):
            for w in range(0, width, 128):
                if first <= col + w < last:
                    at = col + w - first
                    flat_ref[(lane + w) // 128, pl.ds(row, peers, stride=ROWS), :] = values[
                        s * peers : (s + 1) * peers, at : at + 128
                    ]


def from_flat(out_ref, flat_ref):
    for b in range(LANES // 128):
        out_ref[:, b * 128 : (b + 1) * 128] = flat_ref[b].astype(BF16)


def from_tiles(rows_ref, flat_ref, in_ref):
    peers = in_ref.shape[0] // ROWS
    for b in range(LANES // 128):
        flat_ref[b] = in_ref[:, b * 128 : (b + 1) * 128].astype(F32)
    for s in range(SLOTS):
        for row, lane, col, width in pieces(s):
            for w in range(0, width, 128):
                rows_ref[s * peers : (s + 1) * peers, col + w : col + w + 128] = flat_ref[
                    (lane + w) // 128, pl.ds(row, peers, stride=ROWS), :
                ].astype(BF16)


def slot_keys(ids, capacity):
    experts = capacity.shape[1]
    tokens = ids.shape[1]
    expert = iota((experts, tokens), 0)
    named = (ids[0:1, :] == expert) | (ids[1:2, :] == expert)
    earlier = bits(iota((tokens, tokens), 0) < iota((tokens, tokens), 1))
    rank = dot(bits(named), earlier)
    own = iota((experts, experts), 0) == iota((experts, experts), 1)
    limit = jnp.sum(jnp.where(own, capacity.astype(F32), 0.0), axis=1, keepdims=True)
    return jnp.where(named & (rank < limit), rank, NONE)


def combine_weights(v_ref, ids, key, q):
    expert = iota(key.shape, 0)
    scale = q.astype(F32) / 65536.0
    weight = jnp.where(ids[0:1, :] == expert, scale[0:1, :], 0.0) + jnp.where(ids[1:2, :] == expert, scale[1:2, :], 0.0)
    key, weight = key.T, weight.T
    peers = key.shape[1]
    for s in range(SLOTS):
        v_ref[:, s * peers : (s + 1) * peers] = jnp.where(key == float(s), weight, 0.0).astype(BF16)


BLOCK = 256
ONCHIP = pl.BlockSpec(memory_space=pltpu.VMEM)
REMOTE = pl.BlockSpec(memory_space=pltpu.HBM)


def fetch(copies):
    for c in copies:
        c.start()
    return copies


def flat_scratch(rows):
    return pltpu.VMEM((LANES // 128, rows, 128), F32)


def pack_body(ids_ref, cap_ref, q_ref, tok_hbm, w_hbm, out_ref, v_ref, tok_ref, w_ref, pick_ref, flat_ref, sems):
    blocks = w_ref.shape[1] // BLOCK
    get_tok = pltpu.make_async_copy(tok_hbm, tok_ref, sems.at[blocks])
    gets = []
    for n in range(blocks):
        cols = pl.ds(n * BLOCK, BLOCK)
        gets.append(pltpu.make_async_copy(w_hbm.at[:, cols], w_ref.at[:, cols], sems.at[n]))
    fetch([get_tok] + gets)
    ids = ids_ref[...]
    key = slot_keys(ids, cap_ref[...])
    peers = key.shape[0]
    for s in range(SLOTS):
        pick_ref[s * peers : (s + 1) * peers, :] = bits(key == float(s))
    combine_weights(v_ref, ids, key, q_ref[...])
    get_tok.wait()
    for n in range(blocks):
        gets[n].wait()
        sub = dot(tok_ref[...], w_ref[:, n * BLOCK : (n + 1) * BLOCK]).astype(BF16)
        to_flat(flat_ref, dot(pick_ref[...], sub), n * BLOCK)
    from_flat(out_ref, flat_ref)


def split_and_pack(ids, capacity, q, tokens, w_split):
    count = tokens.shape[0]
    experts = capacity.shape[1]
    rows = experts * ROWS
    return pl.pallas_call(
        pack_body,
        in_specs=[ONCHIP] * 3 + [REMOTE] * 2,
        out_specs=[ONCHIP] * 2,
        out_shape=[
            jax.ShapeDtypeStruct((rows, LANES), BF16),
            jax.ShapeDtypeStruct((count, experts * SLOTS), BF16),
        ],
        scratch_shapes=[
            pltpu.VMEM(tokens.shape, BF16),
            pltpu.VMEM(w_split.shape, BF16),
            pltpu.VMEM((experts * SLOTS, count), BF16),
            flat_scratch(rows),
            pltpu.SemaphoreType.DMA((w_split.shape[1] // BLOCK + 1,)),
        ],
        compiler_params=pltpu.CompilerParams(vmem_limit_bytes=62 << 20),
        name="split_pack",
    )(ids, capacity, q, tokens, w_split)


def expert_body(x_ref, in_hbm, down_hbm, out_ref, in_ref, down_ref, rows_ref, act_ref, flat_ref, sems):
    hidden, width = down_ref.shape
    steps = hidden // BLOCK
    gets = []
    for j in range(steps):
        for n, col in enumerate((j * BLOCK, hidden + j * BLOCK)):
            cols = pl.ds(col, BLOCK)
            gets.append(pltpu.make_async_copy(in_hbm.at[0, :, cols], in_ref.at[:, cols], sems.at[2 * j + n]))
    gets.append(pltpu.make_async_copy(down_hbm.at[0], down_ref, sems.at[2 * steps]))
    fetch(gets)
    from_tiles(rows_ref, flat_ref, x_ref)
    rows = rows_ref[...]
    for j in range(steps):
        gets[2 * j].wait()
        gets[2 * j + 1].wait()
        cols = slice(j * BLOCK, (j + 1) * BLOCK)
        gate = dot(rows, in_ref[:, cols])
        up = dot(rows, in_ref[:, hidden + j * BLOCK : hidden + (j + 1) * BLOCK])
        act_ref[:, cols] = (gate / (1.0 + jnp.exp(-gate)) * up).astype(BF16)
    gets[2 * steps].wait()
    for j in range(0, width, BLOCK):
        to_flat(flat_ref, dot(act_ref[...], down_ref[:, j : j + BLOCK]), j)
    from_flat(out_ref, flat_ref)


def expert_rows(tiles, expert_in, expert_out):
    rows = tiles.shape[0]
    slots = rows // ROWS * SLOTS
    width = expert_in.shape[1]
    hidden = expert_out.shape[1]
    return pl.pallas_call(
        expert_body,
        in_specs=[ONCHIP, REMOTE, REMOTE],
        out_specs=ONCHIP,
        out_shape=jax.ShapeDtypeStruct((rows, LANES), BF16),
        scratch_shapes=[
            pltpu.VMEM((width, 2 * hidden), BF16),
            pltpu.VMEM((hidden, width), BF16),
            pltpu.VMEM((slots, width), BF16),
            pltpu.VMEM((slots, hidden), BF16),
            flat_scratch(rows),
            pltpu.SemaphoreType.DMA((2 * hidden // BLOCK + 1,)),
        ],
        compiler_params=pltpu.CompilerParams(vmem_limit_bytes=60 << 20),
        name="experts",
    )(tiles, expert_in, expert_out)


def column_blocks(w_hbm, w_ref, at, sems):
    width = w_hbm.shape[0]
    return fetch(
        [
            pltpu.make_async_copy(w_hbm.at[:, pl.ds(pl.multiple_of(a * width, width), width)], w_ref.at[n], sems.at[n])
            for n, a in enumerate(at)
        ]
    )


def combine_body(at_ref, v_ref, b_ref, w_hbm, head_ref, send_ref, w_ref, rows_ref, flat_ref, sems):
    (get,) = column_blocks(w_hbm, w_ref, [at_ref[0]], sems)
    from_tiles(rows_ref, flat_ref, b_ref)
    head = dot(v_ref[...], rows_ref[...]).astype(BF16)
    head_ref[...] = head
    get.wait()
    send_ref[...] = dot(head, w_ref[0]).astype(BF16)


MERGE = pltpu.CompilerParams(vmem_limit_bytes=48 << 20)


def combine_and_merge(at, v, back, w_merge):
    tokens = v.shape[0]
    width = w_merge.shape[0]
    rows = back.shape[0]
    return pl.pallas_call(
        combine_body,
        in_specs=[pl.BlockSpec(memory_space=pltpu.SMEM), ONCHIP, ONCHIP, REMOTE],
        out_specs=[ONCHIP] * 2,
        out_shape=[jax.ShapeDtypeStruct((tokens, width), BF16)] * 2,
        scratch_shapes=[
            pltpu.VMEM((1, width, width), BF16),
            pltpu.VMEM((rows // ROWS * SLOTS, width), BF16),
            flat_scratch(rows),
            pltpu.SemaphoreType.DMA((1,)),
        ],
        compiler_params=MERGE,
        name="combine_merge",
    )(at, v, back, w_merge)


def merge_body(at_ref, head_ref, w_hbm, far_ref, send_ref, keep_ref, w_ref, sems):
    gets = column_blocks(w_hbm, w_ref, [at_ref[n] for n in (1, 2, 3)], sems)
    head = head_ref[...]
    for n, out_ref in enumerate((far_ref, send_ref, keep_ref)):
        gets[n].wait()
        out_ref[...] = dot(head, w_ref[n]).astype(BF16)


def merge_rest(at, head, w_merge):
    width = w_merge.shape[0]
    return pl.pallas_call(
        merge_body,
        in_specs=[pl.BlockSpec(memory_space=pltpu.SMEM), ONCHIP, REMOTE],
        out_specs=[ONCHIP] * 3,
        out_shape=[jax.ShapeDtypeStruct(head.shape, BF16)] * 3,
        scratch_shapes=[pltpu.VMEM((3, width, width), BF16), pltpu.SemaphoreType.DMA((3,))],
        compiler_params=MERGE,
        name="merge_rest",
    )(at, head, w_merge)


def exchange(tiles, axes):
    peers = tiles.shape[0] // ROWS
    return lax.all_to_all(tiles.reshape(peers, ROWS, LANES), axes, split_axis=0, concat_axis=0, tiled=True).reshape(tiles.shape)


def added(a, b):
    return (a.astype(F32) + b.astype(F32)).astype(BF16)


def body(tokens, w_split, w_merge, expert_in, expert_out, expert_ids, combine_q, capacity):
    ids = expert_ids[0].T
    q = combine_q[0].T
    limit = capacity.reshape(1, -1)
    axes = ("seq", "sub")
    packed, v = split_and_pack(ids, limit, q, tokens, w_split)
    tiles = exchange(packed, axes)
    back = exchange(expert_rows(tiles, expert_in, expert_out), axes)

    me = lax.axis_index("sub")
    core = [(i, i ^ 1) for i in range(4)]
    chip = [(i, i ^ 2) for i in range(4)]
    at = me ^ jnp.array([3, 2, 1, 0], I32)
    head, far_send = combine_and_merge(at, v, back, w_merge)
    far_in = lax.ppermute(far_send, "sub", core)
    far_keep, own_send, own_keep = merge_rest(at, head, w_merge)
    cross = lax.ppermute(added(far_keep, far_in), "sub", chip)
    own_in = lax.ppermute(own_send, "sub", core)
    return (own_keep.astype(F32) + own_in.astype(F32) + cross.astype(F32)).astype(BF16)


def solution(mesh):
    in_specs = (
        P("seq", None),
        P(None, "sub"),
        P("sub", None),
        P(("seq", "sub"), None, None),
        P(("seq", "sub"), None, None),
        P("sub", "seq", None),
        P("sub", "seq", None),
        P(),
    )
    out_specs = P("seq", "sub")
    return jax.shard_map(body, mesh=mesh, in_specs=in_specs, out_specs=out_specs, check_vma=False)
```

```python
import jax
import jax.numpy as jnp
from jax import lax
from jax.experimental import pallas as pl
from jax.experimental.pallas import tpu as pltpu
from jax.sharding import PartitionSpec as P

F32 = jnp.float32
BF16 = jnp.bfloat16
I32 = jnp.int32

SLOTS = 6
ROWS = 8
WIDTH = 1024
LANES = SLOTS * WIDTH // ROWS
NONE = -4.0


def pieces(slot):
    rest = WIDTH - LANES
    return [(slot, 0, 0, LANES), (SLOTS + slot // 3, slot % 3 * rest, LANES, rest)]


SPLIT, EXPERTS, MERGE_MIB = 52, 50, 48


def iota(shape, dim):
    return lax.broadcasted_iota(I32, shape, dim)


def dot(a, b):
    return jnp.dot(a, b, preferred_element_type=F32)


def bits(mask):
    return mask.astype(F32).astype(BF16)


def to_flat(flat_ref, values, first=0):
    peers = values.shape[0] // SLOTS
    last = first + values.shape[1]
    for s in range(SLOTS):
        for row, lane, col, width in pieces(s):
            for w in range(0, width, 128):
                if first <= col + w < last:
                    at = col + w - first
                    flat_ref[(lane + w) // 128, pl.ds(row, peers, stride=ROWS), :] = values[
                        s * peers : (s + 1) * peers, at : at + 128
                    ]


def from_flat(out_ref, flat_ref):
    for b in range(LANES // 128):
        out_ref[:, b * 128 : (b + 1) * 128] = flat_ref[b].astype(BF16)


def from_tiles(rows_ref, flat_ref, in_ref):
    peers = in_ref.shape[0] // ROWS
    for b in range(LANES // 128):
        flat_ref[b] = in_ref[:, b * 128 : (b + 1) * 128].astype(F32)
    for s in range(SLOTS):
        for row, lane, col, width in pieces(s):
            for w in range(0, width, 128):
                rows_ref[s * peers : (s + 1) * peers, col + w : col + w + 128] = flat_ref[
                    (lane + w) // 128, pl.ds(row, peers, stride=ROWS), :
                ].astype(BF16)


def slot_keys(ids, capacity):
    experts = capacity.shape[1]
    tokens = ids.shape[1]
    expert = iota((experts, tokens), 0)
    named = (ids[0:1, :] == expert) | (ids[1:2, :] == expert)
    earlier = bits(iota((tokens, tokens), 0) < iota((tokens, tokens), 1))
    rank = dot(bits(named), earlier)
    own = iota((experts, experts), 0) == iota((experts, experts), 1)
    limit = jnp.sum(jnp.where(own, capacity.astype(F32), 0.0), axis=1, keepdims=True)
    return jnp.where(named & (rank < limit), rank, NONE)


def combine_weights(v_ref, ids, key, q):
    expert = iota(key.shape, 0)
    scale = q.astype(F32) / 65536.0
    weight = jnp.where(ids[0:1, :] == expert, scale[0:1, :], 0.0) + jnp.where(ids[1:2, :] == expert, scale[1:2, :], 0.0)
    key, weight = key.T, weight.T
    peers = key.shape[1]
    for s in range(SLOTS):
        v_ref[:, s * peers : (s + 1) * peers] = jnp.where(key == float(s), weight, 0.0).astype(BF16)


BLOCK = 256
ONCHIP = pl.BlockSpec(memory_space=pltpu.VMEM)
REMOTE = pl.BlockSpec(memory_space=pltpu.HBM)


def fetch(copies):
    for c in copies:
        c.start()
    return copies


def flat_scratch(rows):
    return pltpu.VMEM((LANES // 128, rows, 128), F32)


def pack_body(ids_ref, cap_ref, q_ref, tok_hbm, w_hbm, out_ref, v_ref, tok_ref, w_ref, pick_ref, flat_ref, sems):
    blocks = w_ref.shape[1] // BLOCK
    get_tok = pltpu.make_async_copy(tok_hbm, tok_ref, sems.at[blocks])
    gets = []
    for n in range(blocks):
        cols = pl.ds(n * BLOCK, BLOCK)
        gets.append(pltpu.make_async_copy(w_hbm.at[:, cols], w_ref.at[:, cols], sems.at[n]))
    fetch([get_tok] + gets[:1])
    ids = ids_ref[...]
    key = slot_keys(ids, cap_ref[...])
    peers = key.shape[0]
    for s in range(SLOTS):
        pick_ref[s * peers : (s + 1) * peers, :] = bits(key == float(s))
    combine_weights(v_ref, ids, key, q_ref[...])
    get_tok.wait()
    for n in range(blocks):
        fetch(gets[n + 1 : n + 2])
        gets[n].wait()
        sub = dot(tok_ref[...], w_ref[:, n * BLOCK : (n + 1) * BLOCK]).astype(BF16)
        to_flat(flat_ref, dot(pick_ref[...], sub), n * BLOCK)
    from_flat(out_ref, flat_ref)


def split_and_pack(ids, capacity, q, tokens, w_split):
    count = tokens.shape[0]
    experts = capacity.shape[1]
    rows = experts * ROWS
    return pl.pallas_call(
        pack_body,
        in_specs=[ONCHIP] * 3 + [REMOTE] * 2,
        out_specs=[ONCHIP] * 2,
        out_shape=[
            jax.ShapeDtypeStruct((rows, LANES), BF16),
            jax.ShapeDtypeStruct((count, experts * SLOTS), BF16),
        ],
        scratch_shapes=[
            pltpu.VMEM(tokens.shape, BF16),
            pltpu.VMEM(w_split.shape, BF16),
            pltpu.VMEM((experts * SLOTS, count), BF16),
            flat_scratch(rows),
            pltpu.SemaphoreType.DMA((w_split.shape[1] // BLOCK + 1,)),
        ],
        compiler_params=pltpu.CompilerParams(vmem_limit_bytes=SPLIT << 20),
        name="split_pack",
    )(ids, capacity, q, tokens, w_split)


def expert_body(x_ref, in_hbm, down_hbm, out_ref, in_ref, down_ref, rows_ref, act_ref, flat_ref, sems):
    hidden, width = down_ref.shape
    steps = hidden // BLOCK
    gets = []
    for j in range(steps):
        for n, col in enumerate((j * BLOCK, hidden + j * BLOCK)):
            cols = pl.ds(col, BLOCK)
            gets.append(pltpu.make_async_copy(in_hbm.at[0, :, cols], in_ref.at[:, cols], sems.at[2 * j + n]))
    gets.append(pltpu.make_async_copy(down_hbm.at[0], down_ref, sems.at[2 * steps]))
    fetch(gets[:4])
    from_tiles(rows_ref, flat_ref, x_ref)
    rows = rows_ref[...]
    for j in range(steps):
        fetch(gets[2 * j + 4 : 2 * j + 6])
        gets[2 * j].wait()
        gets[2 * j + 1].wait()
        cols = slice(j * BLOCK, (j + 1) * BLOCK)
        gate = dot(rows, in_ref[:, cols])
        up = dot(rows, in_ref[:, hidden + j * BLOCK : hidden + (j + 1) * BLOCK])
        act_ref[:, cols] = (gate / (1.0 + jnp.exp(-gate)) * up).astype(BF16)
    gets[2 * steps].wait()
    for j in range(0, width, BLOCK):
        to_flat(flat_ref, dot(act_ref[...], down_ref[:, j : j + BLOCK]), j)
    from_flat(out_ref, flat_ref)


def expert_rows(tiles, expert_in, expert_out):
    rows = tiles.shape[0]
    slots = rows // ROWS * SLOTS
    width = expert_in.shape[1]
    hidden = expert_out.shape[1]
    return pl.pallas_call(
        expert_body,
        in_specs=[ONCHIP, REMOTE, REMOTE],
        out_specs=ONCHIP,
        out_shape=jax.ShapeDtypeStruct((rows, LANES), BF16),
        scratch_shapes=[
            pltpu.VMEM((width, 2 * hidden), BF16),
            pltpu.VMEM((hidden, width), BF16),
            pltpu.VMEM((slots, width), BF16),
            pltpu.VMEM((slots, hidden), BF16),
            flat_scratch(rows),
            pltpu.SemaphoreType.DMA((2 * hidden // BLOCK + 1,)),
        ],
        compiler_params=pltpu.CompilerParams(vmem_limit_bytes=EXPERTS << 20),
        name="experts",
    )(tiles, expert_in, expert_out)


def column_blocks(w_hbm, w_ref, order, sems):
    width = w_hbm.shape[0]
    me = lax.axis_index("sub")
    return [
        pltpu.make_async_copy(
            w_hbm.at[:, pl.ds(pl.multiple_of((me ^ other) * width, width), width)], w_ref.at[n], sems.at[n]
        )
        for n, other in enumerate(order)
    ]


def combine_body(v_ref, b_ref, w_hbm, head_ref, send_ref, w_ref, rows_ref, flat_ref, sems):
    (get,) = fetch(column_blocks(w_hbm, w_ref, (3,), sems))
    from_tiles(rows_ref, flat_ref, b_ref)
    head = dot(v_ref[...], rows_ref[...]).astype(BF16)
    head_ref[...] = head
    get.wait()
    send_ref[...] = dot(head, w_ref[0]).astype(BF16)


MERGE = pltpu.CompilerParams(vmem_limit_bytes=MERGE_MIB << 20)


def combine_and_merge(v, back, w_merge):
    tokens = v.shape[0]
    width = w_merge.shape[0]
    rows = back.shape[0]
    return pl.pallas_call(
        combine_body,
        in_specs=[ONCHIP, ONCHIP, REMOTE],
        out_specs=[ONCHIP] * 2,
        out_shape=[jax.ShapeDtypeStruct((tokens, width), BF16)] * 2,
        scratch_shapes=[
            pltpu.VMEM((1, width, width), BF16),
            pltpu.VMEM((rows // ROWS * SLOTS, width), BF16),
            flat_scratch(rows),
            pltpu.SemaphoreType.DMA((1,)),
        ],
        compiler_params=MERGE,
        name="combine_merge",
    )(v, back, w_merge)


def merge_body(head_ref, w_hbm, far_ref, send_ref, keep_ref, w_ref, sems):
    gets = column_blocks(w_hbm, w_ref, (2, 1, 0), sems)
    fetch(gets[:2])
    head = head_ref[...]
    for n, out_ref in enumerate((far_ref, send_ref, keep_ref)):
        gets[n].wait()
        fetch(gets[n + 2 : n + 3])
        out_ref[...] = dot(head, w_ref[n]).astype(BF16)


def merge_rest(head, w_merge):
    width = w_merge.shape[0]
    return pl.pallas_call(
        merge_body,
        in_specs=[ONCHIP, REMOTE],
        out_specs=[ONCHIP] * 3,
        out_shape=[jax.ShapeDtypeStruct(head.shape, BF16)] * 3,
        scratch_shapes=[pltpu.VMEM((3, width, width), BF16), pltpu.SemaphoreType.DMA((3,))],
        compiler_params=MERGE,
        name="merge_rest",
    )(head, w_merge)


def exchange(tiles, axes):
    peers = tiles.shape[0] // ROWS
    return lax.all_to_all(tiles.reshape(peers, ROWS, LANES), axes, split_axis=0, concat_axis=0, tiled=True).reshape(tiles.shape)


def added(a, b):
    return (a.astype(F32) + b.astype(F32)).astype(BF16)


def body(tokens, w_split, w_merge, expert_in, expert_out, expert_ids, combine_q, capacity):
    ids = expert_ids[0].T
    q = combine_q[0].T
    limit = capacity.reshape(1, -1)
    axes = ("seq", "sub")
    packed, v = split_and_pack(ids, limit, q, tokens, w_split)
    tiles = exchange(packed, axes)
    back = exchange(expert_rows(tiles, expert_in, expert_out), axes)

    core = [(i, i ^ 1) for i in range(4)]
    chip = [(i, i ^ 2) for i in range(4)]
    head, far_send = combine_and_merge(v, back, w_merge)
    far_in = lax.ppermute(far_send, "sub", core)
    far_keep, own_send, own_keep = merge_rest(head, w_merge)
    cross = lax.ppermute(added(far_keep, far_in), "sub", chip)
    own_in = lax.ppermute(own_send, "sub", core)
    return (own_keep.astype(F32) + own_in.astype(F32) + cross.astype(F32)).astype(BF16)


def solution(mesh):
    in_specs = (
        P("seq", None),
        P(None, "sub"),
        P("sub", None),
        P(("seq", "sub"), None, None),
        P(("seq", "sub"), None, None),
        P("sub", "seq", None),
        P("sub", "seq", None),
        P(),
    )
    out_specs = P("seq", "sub")
    return jax.shard_map(body, mesh=mesh, in_specs=in_specs, out_specs=out_specs, check_vma=False)
```

```python
import jax
import jax.numpy as jnp
from jax import lax
from jax.experimental import pallas as pl
from jax.experimental.pallas import tpu as pltpu
from jax.sharding import PartitionSpec as P


F32 = jnp.float32
BF16 = jnp.bfloat16
I32 = jnp.int32

SLOTS = 6
ROWS = 8
WIDTH = 1024
LANES = SLOTS * WIDTH // ROWS
NONE = -4.0


def pieces(slot):
    rest = WIDTH - LANES
    return [(slot, 0, 0, LANES), (SLOTS + slot // 3, slot % 3 * rest, LANES, rest)]


SPLIT, EXPERTS, MERGE_MIB = 52, 24, 24


def iota(shape, dim):
    return lax.broadcasted_iota(I32, shape, dim)


def dot(a, b):
    return jnp.dot(a, b, preferred_element_type=F32)


def bits(mask):
    return mask.astype(F32).astype(BF16)


def to_flat(flat_ref, values, first=0):
    peers = values.shape[0] // SLOTS
    last = first + values.shape[1]
    for s in range(SLOTS):
        for row, lane, col, width in pieces(s):
            for w in range(0, width, 128):
                if first <= col + w < last:
                    at = col + w - first
                    flat_ref[(lane + w) // 128, pl.ds(row, peers, stride=ROWS), :] = values[
                        s * peers : (s + 1) * peers, at : at + 128
                    ]


def from_flat(out_ref, flat_ref):
    for b in range(LANES // 128):
        out_ref[:, b * 128 : (b + 1) * 128] = flat_ref[b].astype(BF16)


def from_tiles(rows_ref, flat_ref, in_ref):
    peers = in_ref.shape[0] // ROWS
    for b in range(LANES // 128):
        flat_ref[b] = in_ref[:, b * 128 : (b + 1) * 128].astype(F32)
    for s in range(SLOTS):
        for row, lane, col, width in pieces(s):
            for w in range(0, width, 128):
                rows_ref[s * peers : (s + 1) * peers, col + w : col + w + 128] = flat_ref[
                    (lane + w) // 128, pl.ds(row, peers, stride=ROWS), :
                ].astype(BF16)


def slot_keys(ids, capacity):
    experts = capacity.shape[1]
    tokens = ids.shape[1]
    expert = iota((experts, tokens), 0)
    named = (ids[0:1, :] == expert) | (ids[1:2, :] == expert)
    earlier = bits(iota((tokens, tokens), 0) < iota((tokens, tokens), 1))
    rank = dot(bits(named), earlier)
    own = iota((experts, experts), 0) == iota((experts, experts), 1)
    limit = jnp.sum(jnp.where(own, capacity.astype(F32), 0.0), axis=1, keepdims=True)
    return jnp.where(named & (rank < limit), rank, NONE)


def combine_weights(v_ref, ids, key, q):
    expert = iota(key.shape, 0)
    scale = q.astype(F32) / 65536.0
    weight = jnp.where(ids[0:1, :] == expert, scale[0:1, :], 0.0) + jnp.where(ids[1:2, :] == expert, scale[1:2, :], 0.0)
    key, weight = key.T, weight.T
    peers = key.shape[1]
    for s in range(SLOTS):
        v_ref[:, s * peers : (s + 1) * peers] = jnp.where(key == float(s), weight, 0.0).astype(BF16)


BLOCK = 256
ONCHIP = pl.BlockSpec(memory_space=pltpu.VMEM)
REMOTE = pl.BlockSpec(memory_space=pltpu.HBM)


def fetch(copies):
    for c in copies:
        c.start()
    return copies


def flat_scratch(rows):
    return pltpu.VMEM((LANES // 128, rows, 128), F32)


PARTS = 8


def pack_body(small_ref, tok_hbm, w_hbm, out_ref, v_ref, tok_ref, w_ref, acc_ref, pick_ref, flat_ref, sems):
    part = w_ref.shape[0] // PARTS
    gets = []
    for n in range(PARTS):
        at = pl.ds(n * part, part)
        gets.append(pltpu.make_async_copy(tok_hbm.at[:, at], tok_ref.at[:, at], sems.at[2 * n]))
        gets.append(pltpu.make_async_copy(w_hbm.at[at, :], w_ref.at[at, :], sems.at[2 * n + 1]))
    fetch(gets)
    ids = small_ref[0:2, :]
    peers = pick_ref.shape[0] // SLOTS
    key = slot_keys(ids, small_ref[4:5, :peers])
    for s in range(SLOTS):
        pick_ref[s * peers : (s + 1) * peers, :] = bits(key == float(s))
    combine_weights(v_ref, ids, key, small_ref[2:4, :])
    for n in range(PARTS):
        gets[2 * n].wait()
        gets[2 * n + 1].wait()
        at = slice(n * part, (n + 1) * part)
        product = dot(tok_ref[:, at], w_ref[at, :])
        acc_ref[...] = product if n == 0 else acc_ref[...] + product
    to_flat(flat_ref, dot(pick_ref[...], acc_ref[...].astype(BF16)))
    from_flat(out_ref, flat_ref)


def split_and_pack(ids, capacity, q, tokens, w_split):
    count = tokens.shape[0]
    experts = capacity.shape[0]
    rows = experts * ROWS
    limits = jnp.pad(capacity[None, :], ((0, 0), (0, count - experts)))
    small = jnp.concatenate([ids, q, limits], axis=0)
    return pl.pallas_call(
        pack_body,
        in_specs=[ONCHIP] + [REMOTE] * 2,
        out_specs=[ONCHIP] * 2,
        out_shape=[
            jax.ShapeDtypeStruct((rows, LANES), BF16),
            jax.ShapeDtypeStruct((count, experts * SLOTS), BF16),
        ],
        scratch_shapes=[
            pltpu.VMEM(tokens.shape, BF16),
            pltpu.VMEM(w_split.shape, BF16),
            pltpu.VMEM((count, w_split.shape[1]), F32),
            pltpu.VMEM((experts * SLOTS, count), BF16),
            flat_scratch(rows),
            pltpu.SemaphoreType.DMA((2 * PARTS,)),
        ],
        compiler_params=pltpu.CompilerParams(vmem_limit_bytes=SPLIT << 20),
        name="split_pack",
    )(small, tokens, w_split)


def expert_body(x_ref, in_ref, down_ref, out_ref, rows_ref, act_ref, flat_ref):
    hidden, width = down_ref.shape[1:]
    from_tiles(rows_ref, flat_ref, x_ref)
    rows = rows_ref[...]
    for j in range(0, hidden, BLOCK):
        gate = dot(rows, in_ref[0, :, j : j + BLOCK])
        up = dot(rows, in_ref[0, :, hidden + j : hidden + j + BLOCK])
        act_ref[:, j : j + BLOCK] = (gate / (1.0 + jnp.exp(-gate)) * up).astype(BF16)
    for j in range(0, width, BLOCK):
        to_flat(flat_ref, dot(act_ref[...], down_ref[0, :, j : j + BLOCK]), j)
    from_flat(out_ref, flat_ref)


def expert_rows(tiles, expert_in, expert_out):
    rows = tiles.shape[0]
    slots = rows // ROWS * SLOTS
    width = expert_in.shape[1]
    hidden = expert_out.shape[1]
    return pl.pallas_call(
        expert_body,
        in_specs=[ONCHIP] * 3,
        out_specs=ONCHIP,
        out_shape=jax.ShapeDtypeStruct((rows, LANES), BF16),
        scratch_shapes=[pltpu.VMEM((slots, width), BF16), pltpu.VMEM((slots, hidden), BF16), flat_scratch(rows)],
        compiler_params=pltpu.CompilerParams(vmem_limit_bytes=EXPERTS << 20),
        name="experts",
    )(tiles, expert_in, expert_out)


def column_block(w_ref, other):
    width = w_ref.shape[0]
    return w_ref[:, pl.ds(pl.multiple_of((lax.axis_index("sub") ^ other) * width, width), width)]


MERGE = pltpu.CompilerParams(vmem_limit_bytes=MERGE_MIB << 20)


def combine_body(v_ref, b_ref, w_ref, head_ref, send_ref, rows_ref, flat_ref):
    from_tiles(rows_ref, flat_ref, b_ref)
    head = dot(v_ref[...], rows_ref[...]).astype(BF16)
    head_ref[...] = head
    send_ref[...] = dot(head, column_block(w_ref, 3)).astype(BF16)


def combine_and_merge(v, back, w_merge):
    tokens = v.shape[0]
    width = w_merge.shape[0]
    rows = back.shape[0]
    return pl.pallas_call(
        combine_body,
        in_specs=[ONCHIP] * 3,
        out_specs=[ONCHIP] * 2,
        out_shape=[jax.ShapeDtypeStruct((tokens, width), BF16)] * 2,
        scratch_shapes=[pltpu.VMEM((rows // ROWS * SLOTS, width), BF16), flat_scratch(rows)],
        compiler_params=MERGE,
        name="combine_merge",
    )(v, back, w_merge)


def far_body(head_ref, w_ref, far_ref):
    far_ref[...] = dot(head_ref[...], column_block(w_ref, 2)).astype(BF16)


def merge_far(head, w_merge):
    return pl.pallas_call(
        far_body,
        in_specs=[ONCHIP] * 2,
        out_specs=ONCHIP,
        out_shape=jax.ShapeDtypeStruct(head.shape, BF16),
        compiler_params=MERGE,
        name="merge_far",
    )(head, w_merge)


def own_body(head_ref, w_ref, after_ref, send_ref, keep_ref):
    del after_ref
    head = head_ref[...]
    send_ref[...] = dot(head, column_block(w_ref, 1)).astype(BF16)
    keep_ref[...] = dot(head, column_block(w_ref, 0)).astype(BF16)


def merge_own(head, w_merge, after):
    return pl.pallas_call(
        own_body,
        in_specs=[ONCHIP] * 2 + [REMOTE],
        out_specs=[ONCHIP] * 2,
        out_shape=[jax.ShapeDtypeStruct(head.shape, BF16)] * 2,
        compiler_params=MERGE,
        name="merge_own",
    )(head, w_merge, after)


def exchange(tiles, axes):
    peers = tiles.shape[0] // ROWS
    return lax.all_to_all(tiles.reshape(peers, ROWS, LANES), axes, split_axis=0, concat_axis=0, tiled=True).reshape(tiles.shape)


def added(a, b):
    return (a.astype(F32) + b.astype(F32)).astype(BF16)


def body(tokens, w_split, w_merge, expert_in, expert_out, expert_ids, combine_q, capacity):
    ids = expert_ids[0].T
    q = combine_q[0].T
    axes = ("seq", "sub")
    packed, v = split_and_pack(ids, capacity, q, tokens, w_split)
    tiles = exchange(packed, axes)
    back = exchange(expert_rows(tiles, expert_in, expert_out), axes)

    core = [(i, i ^ 1) for i in range(4)]
    chip = [(i, i ^ 2) for i in range(4)]
    head, far_send = combine_and_merge(v, back, w_merge)
    far_in = lax.ppermute(far_send, "sub", core)
    far_keep = merge_far(head, w_merge)
    far = added(far_keep, far_in)
    cross = lax.ppermute(far, "sub", chip)
    own_send, own_keep = merge_own(head, w_merge, far)
    own_in = lax.ppermute(own_send, "sub", core)
    return (own_keep.astype(F32) + own_in.astype(F32) + cross.astype(F32)).astype(BF16)


def solution(mesh):
    in_specs = (
        P("seq", None),
        P(None, "sub"),
        P("sub", None),
        P(("seq", "sub"), None, None),
        P(("seq", "sub"), None, None),
        P("sub", "seq", None),
        P("sub", "seq", None),
        P(),
    )
    out_specs = P("seq", "sub")
    return jax.shard_map(body, mesh=mesh, in_specs=in_specs, out_specs=out_specs, check_vma=False)
```

```python
import functools

import jax
import jax.numpy as jnp
from jax import lax
from jax.experimental import pallas as pl
from jax.experimental.pallas import tpu as pltpu
from jax.sharding import PartitionSpec as P


F32 = jnp.float32
BF16 = jnp.bfloat16
I32 = jnp.int32

SLOTS = 6
ROWS = 8
WIDTH = 1024
LANES = SLOTS * WIDTH // ROWS
NONE = -4.0


def pieces(slot):
    rest = WIDTH - LANES
    return [(slot, 0, 0, LANES), (SLOTS + slot // 3, slot % 3 * rest, LANES, rest)]


SPLIT, EXPERTS, MERGE_MIB = 52, 24, 24


def iota(shape, dim):
    return lax.broadcasted_iota(I32, shape, dim)


def dot(a, b):
    return jnp.dot(a, b, preferred_element_type=F32)


def bits(mask):
    return mask.astype(F32).astype(BF16)


def to_flat(flat_ref, values, first=0):
    peers = values.shape[0] // SLOTS
    last = first + values.shape[1]
    for s in range(SLOTS):
        for row, lane, col, width in pieces(s):
            for w in range(0, width, 128):
                if first <= col + w < last:
                    at = col + w - first
                    flat_ref[(lane + w) // 128, pl.ds(row, peers, stride=ROWS), :] = values[
                        s * peers : (s + 1) * peers, at : at + 128
                    ]


def from_flat(out_ref, flat_ref):
    for b in range(LANES // 128):
        out_ref[:, b * 128 : (b + 1) * 128] = flat_ref[b].astype(BF16)


def from_tiles(rows_ref, flat_ref, in_ref):
    peers = in_ref.shape[0] // ROWS
    for b in range(LANES // 128):
        flat_ref[b] = in_ref[:, b * 128 : (b + 1) * 128].astype(F32)
    for s in range(SLOTS):
        for row, lane, col, width in pieces(s):
            for w in range(0, width, 128):
                rows_ref[s * peers : (s + 1) * peers, col + w : col + w + 128] = flat_ref[
                    (lane + w) // 128, pl.ds(row, peers, stride=ROWS), :
                ].astype(BF16)


def slot_keys(ids, capacity):
    experts = capacity.shape[1]
    tokens = ids.shape[1]
    expert = iota((experts, tokens), 0)
    named = (ids[0:1, :] == expert) | (ids[1:2, :] == expert)
    earlier = bits(iota((tokens, tokens), 0) < iota((tokens, tokens), 1))
    rank = dot(bits(named), earlier)
    own = iota((experts, experts), 0) == iota((experts, experts), 1)
    limit = jnp.sum(jnp.where(own, capacity.astype(F32), 0.0), axis=1, keepdims=True)
    return jnp.where(named & (rank < limit), rank, NONE)


def combine_weights(v_ref, ids, key, q):
    expert = iota(key.shape, 0)
    scale = q.astype(F32) / 65536.0
    weight = jnp.where(ids[0:1, :] == expert, scale[0:1, :], 0.0) + jnp.where(ids[1:2, :] == expert, scale[1:2, :], 0.0)
    key, weight = key.T, weight.T
    peers = key.shape[1]
    for s in range(SLOTS):
        v_ref[:, s * peers : (s + 1) * peers] = jnp.where(key == float(s), weight, 0.0).astype(BF16)


BLOCK = 256
ONCHIP = pl.BlockSpec(memory_space=pltpu.VMEM)
REMOTE = pl.BlockSpec(memory_space=pltpu.HBM)


def fetch(copies):
    for c in copies:
        c.start()
    return copies


def flat_scratch(rows):
    return pltpu.VMEM((LANES // 128, rows, 128), F32)


PARTS = 8


def pack_body(small_ref, tok_hbm, w_hbm, out_ref, v_ref, tok_ref, w_ref, acc_ref, pick_ref, flat_ref, sems):
    part = w_ref.shape[0] // PARTS
    gets = []
    for n in range(PARTS):
        at = pl.ds(n * part, part)
        gets.append(pltpu.make_async_copy(tok_hbm.at[:, at], tok_ref.at[:, at], sems.at[2 * n]))
        gets.append(pltpu.make_async_copy(w_hbm.at[at, :], w_ref.at[at, :], sems.at[2 * n + 1]))
    fetch(gets)
    ids = small_ref[0:2, :]
    peers = pick_ref.shape[0] // SLOTS
    key = slot_keys(ids, small_ref[4:5, :peers])
    for s in range(SLOTS):
        pick_ref[s * peers : (s + 1) * peers, :] = bits(key == float(s))
    combine_weights(v_ref, ids, key, small_ref[2:4, :])
    for n in range(PARTS):
        gets[2 * n].wait()
        gets[2 * n + 1].wait()
        at = slice(n * part, (n + 1) * part)
        product = dot(tok_ref[:, at], w_ref[at, :])
        acc_ref[...] = product if n == 0 else acc_ref[...] + product
    to_flat(flat_ref, dot(pick_ref[...], acc_ref[...].astype(BF16)))
    from_flat(out_ref, flat_ref)


def split_and_pack(ids, capacity, q, tokens, w_split):
    count = tokens.shape[0]
    experts = capacity.shape[0]
    rows = experts * ROWS
    limits = jnp.pad(capacity[None, :], ((0, 0), (0, count - experts)))
    small = jnp.concatenate([ids, q, limits], axis=0)
    return pl.pallas_call(
        pack_body,
        in_specs=[ONCHIP] + [REMOTE] * 2,
        out_specs=[ONCHIP] * 2,
        out_shape=[
            jax.ShapeDtypeStruct((rows, LANES), BF16),
            jax.ShapeDtypeStruct((count, experts * SLOTS), BF16),
        ],
        scratch_shapes=[
            pltpu.VMEM(tokens.shape, BF16),
            pltpu.VMEM(w_split.shape, BF16),
            pltpu.VMEM((count, w_split.shape[1]), F32),
            pltpu.VMEM((experts * SLOTS, count), BF16),
            flat_scratch(rows),
            pltpu.SemaphoreType.DMA((2 * PARTS,)),
        ],
        compiler_params=pltpu.CompilerParams(vmem_limit_bytes=SPLIT << 20),
        name="split_pack",
    )(small, tokens, w_split)


def expert_body(x_ref, in_ref, down_ref, out_ref, rows_ref, act_ref, flat_ref):
    hidden, width = down_ref.shape[1:]
    from_tiles(rows_ref, flat_ref, x_ref)
    rows = rows_ref[...]
    for j in range(0, hidden, BLOCK):
        gate = dot(rows, in_ref[0, :, j : j + BLOCK])
        up = dot(rows, in_ref[0, :, hidden + j : hidden + j + BLOCK])
        act_ref[:, j : j + BLOCK] = (gate / (1.0 + jnp.exp(-gate)) * up).astype(BF16)
    for j in range(0, width, BLOCK):
        to_flat(flat_ref, dot(act_ref[...], down_ref[0, :, j : j + BLOCK]), j)
    from_flat(out_ref, flat_ref)


def expert_rows(tiles, expert_in, expert_out):
    rows = tiles.shape[0]
    slots = rows // ROWS * SLOTS
    width = expert_in.shape[1]
    hidden = expert_out.shape[1]
    return pl.pallas_call(
        expert_body,
        in_specs=[ONCHIP] * 3,
        out_specs=ONCHIP,
        out_shape=jax.ShapeDtypeStruct((rows, LANES), BF16),
        scratch_shapes=[pltpu.VMEM((slots, width), BF16), pltpu.VMEM((slots, hidden), BF16), flat_scratch(rows)],
        compiler_params=pltpu.CompilerParams(vmem_limit_bytes=EXPERTS << 20),
        name="experts",
    )(tiles, expert_in, expert_out)


def column_block(w_ref, other, half=None):
    width = w_ref.shape[0]
    start = (lax.axis_index("sub") ^ other) * width
    if half is None:
        return w_ref[:, pl.ds(pl.multiple_of(start, width), width)]
    return w_ref[:, pl.ds(pl.multiple_of(start + half * (width // 2), width // 2), width // 2)]


MERGE = pltpu.CompilerParams(vmem_limit_bytes=MERGE_MIB << 20)


def combine_body(v_ref, b_ref, w_ref, head_ref, send_ref, rows_ref, flat_ref):
    from_tiles(rows_ref, flat_ref, b_ref)
    head = dot(v_ref[...], rows_ref[...]).astype(BF16)
    head_ref[...] = head
    send_ref[...] = dot(head, column_block(w_ref, 3, 0)).astype(BF16)


def combine_and_merge(v, back, w_merge):
    tokens = v.shape[0]
    width = w_merge.shape[0]
    rows = back.shape[0]
    return pl.pallas_call(
        combine_body,
        in_specs=[ONCHIP] * 3,
        out_specs=[ONCHIP] * 2,
        out_shape=[
            jax.ShapeDtypeStruct((tokens, width), BF16),
            jax.ShapeDtypeStruct((tokens, width // 2), BF16),
        ],
        scratch_shapes=[pltpu.VMEM((rows // ROWS * SLOTS, width), BF16), flat_scratch(rows)],
        compiler_params=MERGE,
        name="combine_merge",
    )(v, back, w_merge)


def far_body(blocks, head_ref, w_ref, *out_refs):
    for (other, half), out_ref in zip(blocks, out_refs):
        out_ref[...] = dot(head_ref[...], column_block(w_ref, other, half)).astype(BF16)


def merge_far(head, w_merge, blocks):
    tokens, width = head.shape
    return pl.pallas_call(
        functools.partial(far_body, blocks),
        in_specs=[ONCHIP] * 2,
        out_specs=[ONCHIP] * len(blocks),
        out_shape=[jax.ShapeDtypeStruct((tokens, width // 2), BF16)] * len(blocks),
        compiler_params=MERGE,
    )(head, w_merge)


def own_body(head_ref, w_ref, after_ref, send_ref, keep_ref):
    del after_ref
    head = head_ref[...]
    send_ref[...] = dot(head, column_block(w_ref, 1)).astype(BF16)
    keep_ref[...] = dot(head, column_block(w_ref, 0)).astype(BF16)


def merge_own(head, w_merge, after):
    return pl.pallas_call(
        own_body,
        in_specs=[ONCHIP] * 2 + [REMOTE],
        out_specs=[ONCHIP] * 2,
        out_shape=[jax.ShapeDtypeStruct(head.shape, BF16)] * 2,
        compiler_params=MERGE,
        name="merge_own",
    )(head, w_merge, after)


def exchange(tiles, axes):
    peers = tiles.shape[0] // ROWS
    return lax.all_to_all(tiles.reshape(peers, ROWS, LANES), axes, split_axis=0, concat_axis=0, tiled=True).reshape(tiles.shape)


def added(a, b):
    return (a.astype(F32) + b.astype(F32)).astype(BF16)


def body(tokens, w_split, w_merge, expert_in, expert_out, expert_ids, combine_q, capacity):
    ids = expert_ids[0].T
    q = combine_q[0].T
    axes = ("seq", "sub")
    packed, v = split_and_pack(ids, capacity, q, tokens, w_split)
    tiles = exchange(packed, axes)
    back = exchange(expert_rows(tiles, expert_in, expert_out), axes)

    core = [(i, i ^ 1) for i in range(4)]
    chip = [(i, i ^ 2) for i in range(4)]
    head, send_0 = combine_and_merge(v, back, w_merge)
    in_0 = lax.ppermute(send_0, "sub", core)
    (send_1,) = merge_far(head, w_merge, ((3, 1),))
    in_1 = lax.ppermute(send_1, "sub", core)
    keep_0, keep_1 = merge_far(head, w_merge, ((2, 0), (2, 1)))
    far_0 = added(keep_0, in_0)
    cross_0 = lax.ppermute(far_0, "sub", chip)
    far_1 = added(keep_1, in_1)
    cross_1 = lax.ppermute(far_1, "sub", chip)
    own_send, own_keep = merge_own(head, w_merge, far_1)
    own_in = lax.ppermute(own_send, "sub", core)
    cross = jnp.concatenate([cross_0, cross_1], axis=1)
    return (own_keep.astype(F32) + own_in.astype(F32) + cross.astype(F32)).astype(BF16)


def solution(mesh):
    in_specs = (
        P("seq", None),
        P(None, "sub"),
        P("sub", None),
        P(("seq", "sub"), None, None),
        P(("seq", "sub"), None, None),
        P("sub", "seq", None),
        P("sub", "seq", None),
        P(),
    )
    out_specs = P("seq", "sub")
    return jax.shard_map(body, mesh=mesh, in_specs=in_specs, out_specs=out_specs, check_vma=False)
```

```python
import functools

import jax
import jax.numpy as jnp
from jax import lax
from jax.experimental import pallas as pl
from jax.experimental.pallas import tpu as pltpu
from jax.sharding import PartitionSpec as P


F32 = jnp.float32
BF16 = jnp.bfloat16
I32 = jnp.int32

SLOTS = 6
ROWS = 8
WIDTH = 1024
LANES = SLOTS * WIDTH // ROWS
NONE = -4.0


def pieces(slot):
    rest = WIDTH - LANES
    return [(slot, 0, 0, LANES), (SLOTS + slot // 3, slot % 3 * rest, LANES, rest)]


EXPERTS, MERGE_MIB = 24, 24
SPLIT = 52 << 10


def iota(shape, dim):
    return lax.broadcasted_iota(I32, shape, dim)


def dot(a, b):
    return jnp.dot(a, b, preferred_element_type=F32)


def bits(mask):
    return mask.astype(F32).astype(BF16)


def to_flat(flat_ref, values, first=0):
    peers = values.shape[0] // SLOTS
    last = first + values.shape[1]
    for s in range(SLOTS):
        for row, lane, col, width in pieces(s):
            for w in range(0, width, 128):
                if first <= col + w < last:
                    at = col + w - first
                    flat_ref[(lane + w) // 128, pl.ds(row, peers, stride=ROWS), :] = values[
                        s * peers : (s + 1) * peers, at : at + 128
                    ]


def from_flat(out_ref, flat_ref):
    for b in range(LANES // 128):
        out_ref[:, b * 128 : (b + 1) * 128] = flat_ref[b].astype(BF16)


def from_tiles(rows_ref, flat_ref, in_ref):
    peers = in_ref.shape[0] // ROWS
    for b in range(LANES // 128):
        flat_ref[b] = in_ref[:, b * 128 : (b + 1) * 128].astype(F32)
    for s in range(SLOTS):
        for row, lane, col, width in pieces(s):
            for w in range(0, width, 128):
                rows_ref[s * peers : (s + 1) * peers, col + w : col + w + 128] = flat_ref[
                    (lane + w) // 128, pl.ds(row, peers, stride=ROWS), :
                ].astype(BF16)


def slot_keys(ids, capacity):
    experts = capacity.shape[1]
    tokens = ids.shape[1]
    expert = iota((experts, tokens), 0)
    named = (ids[0:1, :] == expert) | (ids[1:2, :] == expert)
    earlier = bits(iota((tokens, tokens), 0) < iota((tokens, tokens), 1))
    rank = dot(bits(named), earlier)
    own = iota((experts, experts), 0) == iota((experts, experts), 1)
    limit = jnp.sum(jnp.where(own, capacity.astype(F32), 0.0), axis=1, keepdims=True)
    return jnp.where(named & (rank < limit), rank, NONE)


def combine_weights(v_ref, ids, key, q):
    expert = iota(key.shape, 0)
    scale = q.astype(F32) / 65536.0
    weight = jnp.where(ids[0:1, :] == expert, scale[0:1, :], 0.0) + jnp.where(ids[1:2, :] == expert, scale[1:2, :], 0.0)
    key, weight = key.T, weight.T
    peers = key.shape[1]
    for s in range(SLOTS):
        v_ref[:, s * peers : (s + 1) * peers] = jnp.where(key == float(s), weight, 0.0).astype(BF16)


BLOCK = 256
ONCHIP = pl.BlockSpec(memory_space=pltpu.VMEM)
REMOTE = pl.BlockSpec(memory_space=pltpu.HBM)


def fetch(copies):
    for c in copies:
        c.start()
    return copies


def flat_scratch(rows):
    return pltpu.VMEM((LANES // 128, rows, 128), F32)


PARTS = 8


def pack_body(
    ids_hbm, cap_hbm, q_hbm, tok_hbm, w_hbm, out_ref, v_ref, ids_ref, cap_ref, q_ref, tok_ref, w_ref, acc_ref, pick_ref,
    flat_ref, sems,
):
    part = w_ref.shape[0] // PARTS
    small = [
        pltpu.make_async_copy(frm, to, sems.at[2 * PARTS + n])
        for n, (frm, to) in enumerate(((ids_hbm, ids_ref), (cap_hbm, cap_ref), (q_hbm, q_ref)))
    ]
    fetch(small)
    gets = []
    for n in range(PARTS):
        at = pl.ds(n * part, part)
        gets.append(pltpu.make_async_copy(tok_hbm.at[:, at], tok_ref.at[:, at], sems.at[2 * n]))
        gets.append(pltpu.make_async_copy(w_hbm.at[at, :], w_ref.at[at, :], sems.at[2 * n + 1]))
    fetch(gets)
    for get in small:
        get.wait()
    ids = ids_ref[...]
    peers = pick_ref.shape[0] // SLOTS
    key = slot_keys(ids, cap_ref[...])
    for s in range(SLOTS):
        pick_ref[s * peers : (s + 1) * peers, :] = bits(key == float(s))
    combine_weights(v_ref, ids, key, q_ref[...])
    for n in range(PARTS):
        gets[2 * n].wait()
        gets[2 * n + 1].wait()
        at = slice(n * part, (n + 1) * part)
        product = dot(tok_ref[:, at], w_ref[at, :])
        acc_ref[...] = product if n == 0 else acc_ref[...] + product
    to_flat(flat_ref, dot(pick_ref[...], acc_ref[...].astype(BF16)))
    from_flat(out_ref, flat_ref)


def split_and_pack(ids, capacity, q, tokens, w_split):
    count = tokens.shape[0]
    limits = capacity[None, :]
    experts = limits.shape[1]
    rows = experts * ROWS
    return pl.pallas_call(
        pack_body,
        in_specs=[REMOTE] * 5,
        out_specs=[ONCHIP] * 2,
        out_shape=[
            jax.ShapeDtypeStruct((rows, LANES), BF16),
            jax.ShapeDtypeStruct((count, experts * SLOTS), BF16),
        ],
        scratch_shapes=[
            pltpu.VMEM(ids.shape, I32),
            pltpu.VMEM(limits.shape, I32),
            pltpu.VMEM(q.shape, I32),
            pltpu.VMEM(tokens.shape, BF16),
            pltpu.VMEM(w_split.shape, BF16),
            pltpu.VMEM((count, w_split.shape[1]), F32),
            pltpu.VMEM((experts * SLOTS, count), BF16),
            flat_scratch(rows),
            pltpu.SemaphoreType.DMA((2 * PARTS + 3,)),
        ],
        compiler_params=pltpu.CompilerParams(vmem_limit_bytes=SPLIT << 10),
        name="split_pack",
    )(*[pltpu.with_memory_space_constraint(a, pltpu.HBM) for a in (ids, limits, q, tokens, w_split)])


def expert_body(x_ref, in_ref, down_ref, out_ref, rows_ref, act_ref, flat_ref):
    hidden, width = down_ref.shape[1:]
    from_tiles(rows_ref, flat_ref, x_ref)
    rows = rows_ref[...]
    for j in range(0, hidden, BLOCK):
        gate = dot(rows, in_ref[0, :, j : j + BLOCK])
        up = dot(rows, in_ref[0, :, hidden + j : hidden + j + BLOCK])
        act_ref[:, j : j + BLOCK] = (gate / (1.0 + jnp.exp(-gate)) * up).astype(BF16)
    for j in range(0, width, BLOCK):
        to_flat(flat_ref, dot(act_ref[...], down_ref[0, :, j : j + BLOCK]), j)
    from_flat(out_ref, flat_ref)


def expert_rows(tiles, expert_in, expert_out):
    rows = tiles.shape[0]
    slots = rows // ROWS * SLOTS
    width = expert_in.shape[1]
    hidden = expert_out.shape[1]
    return pl.pallas_call(
        expert_body,
        in_specs=[ONCHIP] * 3,
        out_specs=ONCHIP,
        out_shape=jax.ShapeDtypeStruct((rows, LANES), BF16),
        scratch_shapes=[pltpu.VMEM((slots, width), BF16), pltpu.VMEM((slots, hidden), BF16), flat_scratch(rows)],
        compiler_params=pltpu.CompilerParams(vmem_limit_bytes=EXPERTS << 20),
        name="experts",
    )(tiles, expert_in, expert_out)


def column_block(w_ref, other, half=None):
    width = w_ref.shape[0]
    start = (lax.axis_index("sub") ^ other) * width
    if half is None:
        return w_ref[:, pl.ds(pl.multiple_of(start, width), width)]
    return w_ref[:, pl.ds(pl.multiple_of(start + half * (width // 2), width // 2), width // 2)]


MERGE = pltpu.CompilerParams(vmem_limit_bytes=MERGE_MIB << 20)


def combine_body(v_ref, b_ref, w_ref, head_ref, send_ref, flat_ref):
    peers = b_ref.shape[0] // ROWS
    for b in range(LANES // 128):
        flat_ref[b] = b_ref[:, b * 128 : (b + 1) * 128].astype(F32)
    head = jnp.zeros(head_ref.shape, F32)
    for first in range(0, SLOTS, 2):
        answers = []
        for s in (first, first + 1):
            parts = [
                flat_ref[(lane + w) // 128, pl.ds(row, peers, stride=ROWS), :].astype(BF16)
                for row, lane, col, width in pieces(s)
                for w in range(0, width, 128)
            ]
            answers.append(jnp.concatenate(parts, axis=1))
        head += dot(v_ref[:, first * peers : (first + 2) * peers], jnp.concatenate(answers, axis=0))
    head = head.astype(BF16)
    head_ref[...] = head
    send_ref[...] = dot(head, column_block(w_ref, 3, 0)).astype(BF16)


def combine_and_merge(v, back, w_merge):
    tokens = v.shape[0]
    width = w_merge.shape[0]
    rows = back.shape[0]
    return pl.pallas_call(
        combine_body,
        in_specs=[ONCHIP] * 3,
        out_specs=[ONCHIP] * 2,
        out_shape=[
            jax.ShapeDtypeStruct((tokens, width), BF16),
            jax.ShapeDtypeStruct((tokens, width // 2), BF16),
        ],
        scratch_shapes=[flat_scratch(rows)],
        compiler_params=MERGE,
        name="combine_merge",
    )(v, back, w_merge)


def far_body(blocks, head_ref, w_ref, *out_refs):
    for (other, half), out_ref in zip(blocks, out_refs):
        out_ref[...] = dot(head_ref[...], column_block(w_ref, other, half)).astype(BF16)


def merge_far(head, w_merge, blocks):
    tokens, width = head.shape
    return pl.pallas_call(
        functools.partial(far_body, blocks),
        in_specs=[ONCHIP] * 2,
        out_specs=[ONCHIP] * len(blocks),
        out_shape=[jax.ShapeDtypeStruct((tokens, width // 2), BF16)] * len(blocks),
        compiler_params=MERGE,
    )(head, w_merge)


def own_body(head_ref, w_ref, after_ref, send_ref, keep_ref):
    del after_ref
    head = head_ref[...]
    send_ref[...] = dot(head, column_block(w_ref, 1)).astype(BF16)
    keep_ref[...] = dot(head, column_block(w_ref, 0)).astype(BF16)


def merge_own(head, w_merge, after):
    return pl.pallas_call(
        own_body,
        in_specs=[ONCHIP] * 2 + [REMOTE],
        out_specs=[ONCHIP] * 2,
        out_shape=[jax.ShapeDtypeStruct(head.shape, BF16)] * 2,
        compiler_params=MERGE,
        name="merge_own",
    )(head, w_merge, after)


def exchange(tiles, axes):
    peers = tiles.shape[0] // ROWS
    return lax.all_to_all(tiles.reshape(peers, ROWS, LANES), axes, split_axis=0, concat_axis=0, tiled=True).reshape(tiles.shape)


def added(a, b):
    return (a.astype(F32) + b.astype(F32)).astype(BF16)


def body(tokens, w_split, w_merge, expert_in, expert_out, expert_ids, combine_q, capacity):
    ids = expert_ids[0].T
    q = combine_q[0].T
    axes = ("seq", "sub")
    packed, v = split_and_pack(ids, capacity, q, tokens, w_split)
    tiles = exchange(packed, axes)
    back = exchange(expert_rows(tiles, expert_in, expert_out), axes)

    core = [(i, i ^ 1) for i in range(4)]
    chip = [(i, i ^ 2) for i in range(4)]
    head, send_0 = combine_and_merge(v, back, w_merge)
    in_0 = lax.ppermute(send_0, "sub", core)
    (send_1,) = merge_far(head, w_merge, ((3, 1),))
    in_1 = lax.ppermute(send_1, "sub", core)
    keep_0, keep_1 = merge_far(head, w_merge, ((2, 0), (2, 1)))
    far_0 = added(keep_0, in_0)
    cross_0 = lax.ppermute(far_0, "sub", chip)
    far_1 = added(keep_1, in_1)
    cross_1 = lax.ppermute(far_1, "sub", chip)
    own_send, own_keep = merge_own(head, w_merge, far_1)
    own_in = lax.ppermute(own_send, "sub", core)
    cross = jnp.concatenate([cross_0, cross_1], axis=1)
    return (own_keep.astype(F32) + own_in.astype(F32) + cross.astype(F32)).astype(BF16)


def solution(mesh):
    in_specs = (
        P("seq", None),
        P(None, "sub"),
        P("sub", None),
        P(("seq", "sub"), None, None),
        P(("seq", "sub"), None, None),
        P("sub", "seq", None),
        P("sub", "seq", None),
        P(),
    )
    out_specs = P("seq", "sub")
    return jax.shard_map(body, mesh=mesh, in_specs=in_specs, out_specs=out_specs, check_vma=False)
```

```python
import functools

import jax
import jax.numpy as jnp
from jax import lax
from jax.experimental import pallas as pl
from jax.experimental.pallas import tpu as pltpu
from jax.sharding import PartitionSpec as P


F32 = jnp.float32
BF16 = jnp.bfloat16
I32 = jnp.int32

SLOTS = 6
ROWS = 8
WIDTH = 1024
LANES = SLOTS * WIDTH // ROWS
NONE = -4.0


def pieces(slot):
    rest = WIDTH - LANES
    return [(slot, 0, 0, LANES), (SLOTS + slot // 3, slot % 3 * rest, LANES, rest)]


EXPERTS, MERGE_MIB = 24, 24
SPLIT = 52 << 10


def iota(shape, dim):
    return lax.broadcasted_iota(I32, shape, dim)


def dot(a, b):
    return jnp.dot(a, b, preferred_element_type=F32)


def bits(mask):
    return mask.astype(F32).astype(BF16)


def to_flat(flat_ref, values, first=0):
    peers = values.shape[0] // SLOTS
    last = first + values.shape[1]
    for s in range(SLOTS):
        for row, lane, col, width in pieces(s):
            for w in range(0, width, 128):
                if first <= col + w < last:
                    at = col + w - first
                    flat_ref[(lane + w) // 128, pl.ds(row, peers, stride=ROWS), :] = values[
                        s * peers : (s + 1) * peers, at : at + 128
                    ]


def from_flat(out_ref, flat_ref):
    for b in range(LANES // 128):
        out_ref[:, b * 128 : (b + 1) * 128] = flat_ref[b].astype(BF16)


def from_tiles(rows_ref, flat_ref, in_ref):
    peers = in_ref.shape[0] // ROWS
    for b in range(LANES // 128):
        flat_ref[b] = in_ref[:, b * 128 : (b + 1) * 128].astype(F32)
    for s in range(SLOTS):
        for row, lane, col, width in pieces(s):
            for w in range(0, width, 128):
                rows_ref[s * peers : (s + 1) * peers, col + w : col + w + 128] = flat_ref[
                    (lane + w) // 128, pl.ds(row, peers, stride=ROWS), :
                ].astype(BF16)


def slot_keys(ids, capacity):
    experts = capacity.shape[1]
    tokens = ids.shape[1]
    expert = iota((experts, tokens), 0)
    named = (ids[0:1, :] == expert) | (ids[1:2, :] == expert)
    earlier = bits(iota((tokens, tokens), 0) < iota((tokens, tokens), 1))
    rank = dot(bits(named), earlier)
    own = iota((experts, experts), 0) == iota((experts, experts), 1)
    limit = jnp.sum(jnp.where(own, capacity.astype(F32), 0.0), axis=1, keepdims=True)
    return jnp.where(named & (rank < limit), rank, NONE)


def combine_weights(v_ref, ids, key, q):
    expert = iota(key.shape, 0)
    scale = q.astype(F32) / 65536.0
    weight = jnp.where(ids[0:1, :] == expert, scale[0:1, :], 0.0) + jnp.where(ids[1:2, :] == expert, scale[1:2, :], 0.0)
    key, weight = key.T, weight.T
    peers = key.shape[1]
    for s in range(SLOTS):
        v_ref[:, s * peers : (s + 1) * peers] = jnp.where(key == float(s), weight, 0.0).astype(BF16)


BLOCK = 256
ONCHIP = pl.BlockSpec(memory_space=pltpu.VMEM)
REMOTE = pl.BlockSpec(memory_space=pltpu.HBM)


def fetch(copies):
    for c in copies:
        c.start()
    return copies


def flat_scratch(rows):
    return pltpu.VMEM((LANES // 128, rows, 128), F32)


PARTS = 8


def pack_body(
    ids_hbm, cap_hbm, q_hbm, tok_hbm, w_hbm, out_ref, v_ref, ids_ref, cap_ref, q_ref, tok_ref, w_ref, acc_ref, pick_ref,
    flat_ref, sems,
):
    part = w_ref.shape[0] // PARTS
    small = [
        pltpu.make_async_copy(frm, to, sems.at[2 * PARTS + n])
        for n, (frm, to) in enumerate(((ids_hbm, ids_ref), (cap_hbm, cap_ref), (q_hbm, q_ref)))
    ]
    fetch(small)
    gets = []
    for n in range(PARTS):
        at = pl.ds(n * part, part)
        gets.append(pltpu.make_async_copy(tok_hbm.at[:, at], tok_ref.at[:, at], sems.at[2 * n]))
        gets.append(pltpu.make_async_copy(w_hbm.at[at, :], w_ref.at[at, :], sems.at[2 * n + 1]))
    fetch(gets)
    for get in small:
        get.wait()
    ids = ids_ref[...]
    peers = pick_ref.shape[0] // SLOTS
    key = slot_keys(ids, cap_ref[...])
    for s in range(SLOTS):
        pick_ref[s * peers : (s + 1) * peers, :] = bits(key == float(s))
    combine_weights(v_ref, ids, key, q_ref[...])
    for n in range(PARTS):
        gets[2 * n].wait()
        gets[2 * n + 1].wait()
        at = slice(n * part, (n + 1) * part)
        product = dot(tok_ref[:, at], w_ref[at, :])
        acc_ref[...] = product if n == 0 else acc_ref[...] + product
    to_flat(flat_ref, dot(pick_ref[...], acc_ref[...].astype(BF16)))
    from_flat(out_ref, flat_ref)


def split_and_pack(ids, capacity, q, tokens, w_split):
    count = tokens.shape[0]
    limits = capacity[None, :]
    experts = limits.shape[1]
    rows = experts * ROWS
    return pl.pallas_call(
        pack_body,
        in_specs=[REMOTE] * 5,
        out_specs=[ONCHIP] * 2,
        out_shape=[
            jax.ShapeDtypeStruct((rows, LANES), BF16),
            jax.ShapeDtypeStruct((count, experts * SLOTS), BF16),
        ],
        scratch_shapes=[
            pltpu.VMEM(ids.shape, I32),
            pltpu.VMEM(limits.shape, I32),
            pltpu.VMEM(q.shape, I32),
            pltpu.VMEM(tokens.shape, BF16),
            pltpu.VMEM(w_split.shape, BF16),
            pltpu.VMEM((count, w_split.shape[1]), F32),
            pltpu.VMEM((experts * SLOTS, count), BF16),
            flat_scratch(rows),
            pltpu.SemaphoreType.DMA((2 * PARTS + 3,)),
        ],
        compiler_params=pltpu.CompilerParams(vmem_limit_bytes=SPLIT << 10),
        name="split_pack",
    )(*[pltpu.with_memory_space_constraint(a, pltpu.HBM) for a in (ids, limits, q, tokens, w_split)])


def expert_body(x_ref, in_ref, down_ref, out_ref, rows_ref, act_ref, flat_ref):
    hidden, width = down_ref.shape[1:]
    from_tiles(rows_ref, flat_ref, x_ref)
    rows = rows_ref[...]
    for j in range(0, hidden, BLOCK):
        gate = dot(rows, in_ref[0, :, j : j + BLOCK])
        up = dot(rows, in_ref[0, :, hidden + j : hidden + j + BLOCK])
        act_ref[:, j : j + BLOCK] = (gate / (1.0 + jnp.exp(-gate)) * up).astype(BF16)
    for j in range(0, width, BLOCK):
        to_flat(flat_ref, dot(act_ref[...], down_ref[0, :, j : j + BLOCK]), j)
    from_flat(out_ref, flat_ref)


def expert_rows(tiles, expert_in, expert_out):
    rows = tiles.shape[0]
    slots = rows // ROWS * SLOTS
    width = expert_in.shape[1]
    hidden = expert_out.shape[1]
    return pl.pallas_call(
        expert_body,
        in_specs=[ONCHIP] * 3,
        out_specs=ONCHIP,
        out_shape=jax.ShapeDtypeStruct((rows, LANES), BF16),
        scratch_shapes=[pltpu.VMEM((slots, width), BF16), pltpu.VMEM((slots, hidden), BF16), flat_scratch(rows)],
        compiler_params=pltpu.CompilerParams(vmem_limit_bytes=EXPERTS << 20),
        name="experts",
    )(tiles, expert_in, expert_out)


FIRST = 256


def column_block(w_ref, other, half=None):
    width = w_ref.shape[0]
    start, size = {None: (0, width), 0: (0, FIRST), 1: (FIRST, width - FIRST)}[half]
    return w_ref[:, pl.ds(pl.multiple_of((lax.axis_index("sub") ^ other) * width + start, 128), size)]


MERGE = pltpu.CompilerParams(vmem_limit_bytes=MERGE_MIB << 20)


def combine_body(v_ref, b_ref, w_ref, head_ref, send_ref, keep_ref, flat_ref):
    peers = b_ref.shape[0] // ROWS
    for b in range(LANES // 128):
        flat_ref[b] = b_ref[:, b * 128 : (b + 1) * 128].astype(F32)
    head = jnp.zeros(head_ref.shape, F32)
    for first in range(0, SLOTS, 2):
        answers = []
        for s in (first, first + 1):
            parts = [
                flat_ref[(lane + w) // 128, pl.ds(row, peers, stride=ROWS), :].astype(BF16)
                for row, lane, col, width in pieces(s)
                for w in range(0, width, 128)
            ]
            answers.append(jnp.concatenate(parts, axis=1))
        head += dot(v_ref[:, first * peers : (first + 2) * peers], jnp.concatenate(answers, axis=0))
    head = head.astype(BF16)
    head_ref[...] = head
    send_ref[...] = dot(head, column_block(w_ref, 3, 0)).astype(BF16)
    keep_ref[...] = dot(head, column_block(w_ref, 2, 0)).astype(BF16)


def combine_and_merge(v, back, w_merge):
    tokens = v.shape[0]
    width = w_merge.shape[0]
    rows = back.shape[0]
    return pl.pallas_call(
        combine_body,
        in_specs=[ONCHIP] * 3,
        out_specs=[ONCHIP] * 3,
        out_shape=[
            jax.ShapeDtypeStruct((tokens, width), BF16),
            jax.ShapeDtypeStruct((tokens, FIRST), BF16),
            jax.ShapeDtypeStruct((tokens, FIRST), BF16),
        ],
        scratch_shapes=[flat_scratch(rows)],
        compiler_params=MERGE,
        name="combine_merge",
    )(v, back, w_merge)


def far_body(blocks, head_ref, w_ref, *out_refs):
    for (other, half), out_ref in zip(blocks, out_refs):
        out_ref[...] = dot(head_ref[...], column_block(w_ref, other, half)).astype(BF16)


def merge_far(head, w_merge, blocks):
    tokens, width = head.shape
    return pl.pallas_call(
        functools.partial(far_body, blocks),
        in_specs=[ONCHIP] * 2,
        out_specs=[ONCHIP] * len(blocks),
        out_shape=[jax.ShapeDtypeStruct((tokens, (FIRST, width - FIRST)[half]), BF16) for _, half in blocks],
        compiler_params=MERGE,
    )(head, w_merge)


def own_body(head_ref, w_ref, after_ref, send_ref, keep_ref):
    del after_ref
    head = head_ref[...]
    send_ref[...] = dot(head, column_block(w_ref, 1)).astype(BF16)
    keep_ref[...] = dot(head, column_block(w_ref, 0)).astype(BF16)


def merge_own(head, w_merge, after):
    return pl.pallas_call(
        own_body,
        in_specs=[ONCHIP] * 2 + [REMOTE],
        out_specs=[ONCHIP] * 2,
        out_shape=[jax.ShapeDtypeStruct(head.shape, BF16)] * 2,
        compiler_params=MERGE,
        name="merge_own",
    )(head, w_merge, after)


def exchange(tiles, axes):
    peers = tiles.shape[0] // ROWS
    return lax.all_to_all(tiles.reshape(peers, ROWS, LANES), axes, split_axis=0, concat_axis=0, tiled=True).reshape(tiles.shape)


def added(a, b):
    return (a.astype(F32) + b.astype(F32)).astype(BF16)


def body(tokens, w_split, w_merge, expert_in, expert_out, expert_ids, combine_q, capacity):
    ids = expert_ids[0].T
    q = combine_q[0].T
    axes = ("seq", "sub")
    packed, v = split_and_pack(ids, capacity, q, tokens, w_split)
    tiles = exchange(packed, axes)
    back = exchange(expert_rows(tiles, expert_in, expert_out), axes)

    core = [(i, i ^ 1) for i in range(4)]
    chip = [(i, i ^ 2) for i in range(4)]
    head, send_0, keep_0 = combine_and_merge(v, back, w_merge)
    in_0 = lax.ppermute(send_0, "sub", core)
    (send_1,) = merge_far(head, w_merge, ((3, 1),))
    in_1 = lax.ppermute(send_1, "sub", core)
    (keep_1,) = merge_far(head, w_merge, ((2, 1),))
    far_0 = added(keep_0, in_0)
    cross_0 = lax.ppermute(far_0, "sub", chip)
    far_1 = added(keep_1, in_1)
    cross_1 = lax.ppermute(far_1, "sub", chip)
    own_send, own_keep = merge_own(head, w_merge, far_1)
    own_in = lax.ppermute(own_send, "sub", core)
    cross = jnp.concatenate([cross_0, cross_1], axis=1)
    return (own_keep.astype(F32) + own_in.astype(F32) + cross.astype(F32)).astype(BF16)


def solution(mesh):
    in_specs = (
        P("seq", None),
        P(None, "sub"),
        P("sub", None),
        P(("seq", "sub"), None, None),
        P(("seq", "sub"), None, None),
        P("sub", "seq", None),
        P("sub", "seq", None),
        P(),
    )
    out_specs = P("seq", "sub")
    return jax.shard_map(body, mesh=mesh, in_specs=in_specs, out_specs=out_specs, check_vma=False)
```

```python
import functools

import jax
import jax.numpy as jnp
from jax import lax
from jax.experimental import pallas as pl
from jax.experimental.pallas import tpu as pltpu
from jax.sharding import PartitionSpec as P


F32 = jnp.float32
BF16 = jnp.bfloat16
I32 = jnp.int32

SLOTS = 6
ROWS = 8
WIDTH = 1024
LANES = SLOTS * WIDTH // ROWS
NONE = -4.0


def pieces(slot):
    rest = WIDTH - LANES
    return [(slot, 0, 0, LANES), (SLOTS + slot // 3, slot % 3 * rest, LANES, rest)]


EXPERTS, MERGE_MIB = 24, 24
SPLIT = 52 << 10


def iota(shape, dim):
    return lax.broadcasted_iota(I32, shape, dim)


def dot(a, b):
    return jnp.dot(a, b, preferred_element_type=F32)


def bits(mask):
    return mask.astype(F32).astype(BF16)


def to_flat(flat_ref, values, first=0):
    peers = values.shape[0] // SLOTS
    last = first + values.shape[1]
    for s in range(SLOTS):
        for row, lane, col, width in pieces(s):
            for w in range(0, width, 128):
                if first <= col + w < last:
                    at = col + w - first
                    flat_ref[(lane + w) // 128, pl.ds(row, peers, stride=ROWS), :] = values[
                        s * peers : (s + 1) * peers, at : at + 128
                    ]


def from_flat(out_ref, flat_ref):
    for b in range(LANES // 128):
        out_ref[:, b * 128 : (b + 1) * 128] = flat_ref[b].astype(BF16)


def from_tiles(rows_ref, flat_ref, in_ref):
    peers = in_ref.shape[0] // ROWS
    for b in range(LANES // 128):
        flat_ref[b] = in_ref[:, b * 128 : (b + 1) * 128].astype(F32)
    for s in range(SLOTS):
        for row, lane, col, width in pieces(s):
            for w in range(0, width, 128):
                rows_ref[s * peers : (s + 1) * peers, col + w : col + w + 128] = flat_ref[
                    (lane + w) // 128, pl.ds(row, peers, stride=ROWS), :
                ].astype(BF16)


def slot_keys(ids, capacity):
    experts = capacity.shape[1]
    tokens = ids.shape[1]
    expert = iota((experts, tokens), 0)
    named = (ids[0:1, :] == expert) | (ids[1:2, :] == expert)
    earlier = bits(iota((tokens, tokens), 0) < iota((tokens, tokens), 1))
    rank = dot(bits(named), earlier)
    own = iota((experts, experts), 0) == iota((experts, experts), 1)
    limit = jnp.sum(jnp.where(own, capacity.astype(F32), 0.0), axis=1, keepdims=True)
    return jnp.where(named & (rank < limit), rank, NONE)


def combine_weights(v_ref, ids, key, q):
    expert = iota(key.shape, 0)
    scale = q.astype(F32) / 65536.0
    weight = jnp.where(ids[0:1, :] == expert, scale[0:1, :], 0.0) + jnp.where(ids[1:2, :] == expert, scale[1:2, :], 0.0)
    key, weight = key.T, weight.T
    peers = key.shape[1]
    for s in range(SLOTS):
        v_ref[:, s * peers : (s + 1) * peers] = jnp.where(key == float(s), weight, 0.0).astype(BF16)


BLOCK = 256
ONCHIP = pl.BlockSpec(memory_space=pltpu.VMEM)
REMOTE = pl.BlockSpec(memory_space=pltpu.HBM)


def fetch(copies):
    for c in copies:
        c.start()
    return copies


def flat_scratch(rows):
    return pltpu.VMEM((LANES // 128, rows, 128), F32)


PARTS = 8


def pack_body(
    ids_hbm, cap_hbm, q_hbm, tok_hbm, w_hbm, out_ref, v_ref, ids_ref, cap_ref, q_ref, tok_ref, w_ref, acc_ref, pick_ref,
    flat_ref, sems,
):
    part = w_ref.shape[0] // PARTS
    small = [
        pltpu.make_async_copy(frm, to, sems.at[2 * PARTS + n])
        for n, (frm, to) in enumerate(((ids_hbm, ids_ref), (cap_hbm, cap_ref), (q_hbm, q_ref)))
    ]
    fetch(small)
    gets = []
    for n in range(PARTS):
        at = pl.ds(n * part, part)
        gets.append(pltpu.make_async_copy(tok_hbm.at[:, at], tok_ref.at[:, at], sems.at[2 * n]))
        gets.append(pltpu.make_async_copy(w_hbm.at[at, :], w_ref.at[at, :], sems.at[2 * n + 1]))
    fetch(gets)
    for get in small:
        get.wait()
    ids = ids_ref[...]
    peers = pick_ref.shape[0] // SLOTS
    key = slot_keys(ids, cap_ref[...])
    for s in range(SLOTS):
        pick_ref[s * peers : (s + 1) * peers, :] = bits(key == float(s))
    combine_weights(v_ref, ids, key, q_ref[...])
    for n in range(PARTS):
        gets[2 * n].wait()
        gets[2 * n + 1].wait()
        at = slice(n * part, (n + 1) * part)
        product = dot(tok_ref[:, at], w_ref[at, :])
        acc_ref[...] = product if n == 0 else acc_ref[...] + product
    to_flat(flat_ref, dot(pick_ref[...], acc_ref[...].astype(BF16)))
    from_flat(out_ref, flat_ref)


def split_and_pack(ids, capacity, q, tokens, w_split):
    count = tokens.shape[0]
    limits = capacity[None, :]
    experts = limits.shape[1]
    rows = experts * ROWS
    return pl.pallas_call(
        pack_body,
        in_specs=[REMOTE] * 5,
        out_specs=[ONCHIP] * 2,
        out_shape=[
            jax.ShapeDtypeStruct((rows, LANES), BF16),
            jax.ShapeDtypeStruct((count, experts * SLOTS), BF16),
        ],
        scratch_shapes=[
            pltpu.VMEM(ids.shape, I32),
            pltpu.VMEM(limits.shape, I32),
            pltpu.VMEM(q.shape, I32),
            pltpu.VMEM(tokens.shape, BF16),
            pltpu.VMEM(w_split.shape, BF16),
            pltpu.VMEM((count, w_split.shape[1]), F32),
            pltpu.VMEM((experts * SLOTS, count), BF16),
            flat_scratch(rows),
            pltpu.SemaphoreType.DMA((2 * PARTS + 3,)),
        ],
        compiler_params=pltpu.CompilerParams(vmem_limit_bytes=SPLIT << 10),
        name="split_pack",
    )(*[pltpu.with_memory_space_constraint(a, pltpu.HBM) for a in (ids, limits, q, tokens, w_split)])


def expert_body(x_ref, in_ref, down_ref, out_ref, rows_ref, act_ref, flat_ref):
    hidden, width = down_ref.shape[1:]
    from_tiles(rows_ref, flat_ref, x_ref)
    rows = rows_ref[...]
    for j in range(0, hidden, BLOCK):
        gate = dot(rows, in_ref[0, :, j : j + BLOCK])
        up = dot(rows, in_ref[0, :, hidden + j : hidden + j + BLOCK])
        act_ref[:, j : j + BLOCK] = (gate / (1.0 + jnp.exp(-gate)) * up).astype(BF16)
    for j in range(0, width, BLOCK):
        to_flat(flat_ref, dot(act_ref[...], down_ref[0, :, j : j + BLOCK]), j)
    from_flat(out_ref, flat_ref)


def expert_rows(tiles, expert_in, expert_out):
    rows = tiles.shape[0]
    slots = rows // ROWS * SLOTS
    width = expert_in.shape[1]
    hidden = expert_out.shape[1]
    return pl.pallas_call(
        expert_body,
        in_specs=[ONCHIP] * 3,
        out_specs=ONCHIP,
        out_shape=jax.ShapeDtypeStruct((rows, LANES), BF16),
        scratch_shapes=[pltpu.VMEM((slots, width), BF16), pltpu.VMEM((slots, hidden), BF16), flat_scratch(rows)],
        compiler_params=pltpu.CompilerParams(vmem_limit_bytes=EXPERTS << 20),
        name="experts",
    )(tiles, expert_in, expert_out)


FIRST = 256


def column_block(w_ref, other, half=None):
    width = w_ref.shape[0]
    start, size = {None: (0, width), 0: (0, FIRST), 1: (FIRST, width - FIRST)}[half]
    return w_ref[:, pl.ds(pl.multiple_of((lax.axis_index("sub") ^ other) * width + start, 128), size)]


MERGE = pltpu.CompilerParams(vmem_limit_bytes=MERGE_MIB << 20)


def combine_body(v_ref, b_ref, w_ref, head_ref, send_ref, keep_ref, flat_ref):
    peers = b_ref.shape[0] // ROWS
    for b in range(LANES // 128):
        flat_ref[b] = b_ref[:, b * 128 : (b + 1) * 128].astype(F32)
    head = jnp.zeros(head_ref.shape, F32)
    for first in range(0, SLOTS, 2):
        answers = []
        for s in (first, first + 1):
            parts = [
                flat_ref[(lane + w) // 128, pl.ds(row, peers, stride=ROWS), :].astype(BF16)
                for row, lane, col, width in pieces(s)
                for w in range(0, width, 128)
            ]
            answers.append(jnp.concatenate(parts, axis=1))
        head += dot(v_ref[:, first * peers : (first + 2) * peers], jnp.concatenate(answers, axis=0))
    head = head.astype(BF16)
    head_ref[...] = head
    send_ref[...] = dot(head, column_block(w_ref, 3, 0)).astype(BF16)
    keep_ref[...] = dot(head, column_block(w_ref, 2, 0)).astype(BF16)


def combine_and_merge(v, back, w_merge):
    tokens = v.shape[0]
    width = w_merge.shape[0]
    rows = back.shape[0]
    return pl.pallas_call(
        combine_body,
        in_specs=[ONCHIP] * 3,
        out_specs=[ONCHIP] * 3,
        out_shape=[
            jax.ShapeDtypeStruct((tokens, width), BF16),
            jax.ShapeDtypeStruct((tokens, FIRST), BF16),
            jax.ShapeDtypeStruct((tokens, FIRST), BF16),
        ],
        scratch_shapes=[flat_scratch(rows)],
        compiler_params=MERGE,
        name="combine_merge",
    )(v, back, w_merge)


def far_body(blocks, head_ref, w_ref, *out_refs):
    for (other, half), out_ref in zip(blocks, out_refs):
        out_ref[...] = dot(head_ref[...], column_block(w_ref, other, half)).astype(BF16)


def merge_far(head, w_merge, blocks):
    tokens, width = head.shape
    return pl.pallas_call(
        functools.partial(far_body, blocks),
        in_specs=[ONCHIP] * 2,
        out_specs=[ONCHIP] * len(blocks),
        out_shape=[jax.ShapeDtypeStruct((tokens, (FIRST, width - FIRST)[half]), BF16) for _, half in blocks],
        compiler_params=MERGE,
    )(head, w_merge)


def own_body(head_ref, w_ref, after_ref, send_ref, keep_ref):
    del after_ref
    head = head_ref[...]
    send_ref[...] = dot(head, column_block(w_ref, 1)).astype(BF16)
    keep_ref[...] = dot(head, column_block(w_ref, 0)).astype(BF16)


def merge_own(head, w_merge, after):
    return pl.pallas_call(
        own_body,
        in_specs=[ONCHIP] * 2 + [REMOTE],
        out_specs=[ONCHIP] * 2,
        out_shape=[jax.ShapeDtypeStruct(head.shape, BF16)] * 2,
        compiler_params=MERGE,
        name="merge_own",
    )(head, w_merge, after)


WRITES = 4


def last_body(keep_ref, in_ref, cross_0_ref, cross_1_ref, out_hbm, sum_ref, sems):
    rows = sum_ref.shape[0] // WRITES
    puts = []
    for n in range(WRITES):
        at = slice(n * rows, (n + 1) * rows)
        own = keep_ref[at, :].astype(F32) + in_ref[at, :].astype(F32)
        sum_ref[at, :FIRST] = (own[:, :FIRST] + cross_0_ref[at, :].astype(F32)).astype(BF16)
        sum_ref[at, FIRST:] = (own[:, FIRST:] + cross_1_ref[at, :].astype(F32)).astype(BF16)
        piece = pl.ds(n * rows, rows)
        puts += fetch([pltpu.make_async_copy(sum_ref.at[piece, :], out_hbm.at[piece, :], sems.at[n])])
    for put in puts:
        put.wait()


def last_sum(own_keep, own_in, cross_0, cross_1):
    return pl.pallas_call(
        last_body,
        in_specs=[ONCHIP] * 4,
        out_specs=REMOTE,
        out_shape=jax.ShapeDtypeStruct(own_keep.shape, BF16),
        scratch_shapes=[pltpu.VMEM(own_keep.shape, BF16), pltpu.SemaphoreType.DMA((WRITES,))],
        compiler_params=MERGE,
        name="last_sum",
    )(own_keep, own_in, cross_0, cross_1)


def exchange(tiles, axes):
    peers = tiles.shape[0] // ROWS
    return lax.all_to_all(tiles.reshape(peers, ROWS, LANES), axes, split_axis=0, concat_axis=0, tiled=True).reshape(tiles.shape)


def added(a, b):
    return (a.astype(F32) + b.astype(F32)).astype(BF16)


def body(tokens, w_split, w_merge, expert_in, expert_out, expert_ids, combine_q, capacity):
    ids = expert_ids[0].T
    q = combine_q[0].T
    axes = ("seq", "sub")
    packed, v = split_and_pack(ids, capacity, q, tokens, w_split)
    tiles = exchange(packed, axes)
    back = exchange(expert_rows(tiles, expert_in, expert_out), axes)

    core = [(i, i ^ 1) for i in range(4)]
    chip = [(i, i ^ 2) for i in range(4)]
    head, send_0, keep_0 = combine_and_merge(v, back, w_merge)
    in_0 = lax.ppermute(send_0, "sub", core)
    (send_1,) = merge_far(head, w_merge, ((3, 1),))
    in_1 = lax.ppermute(send_1, "sub", core)
    (keep_1,) = merge_far(head, w_merge, ((2, 1),))
    far_0 = added(keep_0, in_0)
    cross_0 = lax.ppermute(far_0, "sub", chip)
    far_1 = added(keep_1, in_1)
    cross_1 = lax.ppermute(far_1, "sub", chip)
    own_send, own_keep = merge_own(head, w_merge, far_1)
    own_in = lax.ppermute(own_send, "sub", core)
    return last_sum(own_keep, own_in, cross_0, cross_1)


def solution(mesh):
    in_specs = (
        P("seq", None),
        P(None, "sub"),
        P("sub", None),
        P(("seq", "sub"), None, None),
        P(("seq", "sub"), None, None),
        P("sub", "seq", None),
        P("sub", "seq", None),
        P(),
    )
    out_specs = P("seq", "sub")
    return jax.shard_map(body, mesh=mesh, in_specs=in_specs, out_specs=out_specs, check_vma=False)
```

```python
import functools

import jax
import jax.numpy as jnp
from jax import lax
from jax.experimental import pallas as pl
from jax.experimental.pallas import tpu as pltpu
from jax.sharding import PartitionSpec as P


F32 = jnp.float32
BF16 = jnp.bfloat16
I32 = jnp.int32

SLOTS = 6
ROWS = 8
WIDTH = 1024
LANES = SLOTS * WIDTH // ROWS
NONE = -4.0


def pieces(slot):
    rest = WIDTH - LANES
    return [(slot, 0, 0, LANES), (SLOTS + slot // 3, slot % 3 * rest, LANES, rest)]


EXPERTS, MERGE_MIB = 24, 24
SPLIT = 52 << 10


def iota(shape, dim):
    return lax.broadcasted_iota(I32, shape, dim)


def dot(a, b):
    return jnp.dot(a, b, preferred_element_type=F32)


def bits(mask):
    return mask.astype(F32).astype(BF16)


def to_flat(flat_ref, values, first=0):
    peers = values.shape[0] // SLOTS
    last = first + values.shape[1]
    for s in range(SLOTS):
        for row, lane, col, width in pieces(s):
            for w in range(0, width, 128):
                if first <= col + w < last:
                    at = col + w - first
                    flat_ref[(lane + w) // 128, pl.ds(row, peers, stride=ROWS), :] = values[
                        s * peers : (s + 1) * peers, at : at + 128
                    ]


def from_flat(out_ref, flat_ref):
    for b in range(LANES // 128):
        out_ref[:, b * 128 : (b + 1) * 128] = flat_ref[b].astype(BF16)


def from_tiles(rows_ref, flat_ref, in_ref):
    peers = in_ref.shape[0] // ROWS
    for b in range(LANES // 128):
        flat_ref[b] = in_ref[:, b * 128 : (b + 1) * 128].astype(F32)
    for s in range(SLOTS):
        for row, lane, col, width in pieces(s):
            for w in range(0, width, 128):
                rows_ref[s * peers : (s + 1) * peers, col + w : col + w + 128] = flat_ref[
                    (lane + w) // 128, pl.ds(row, peers, stride=ROWS), :
                ].astype(BF16)


def slot_keys(ids, capacity):
    experts = capacity.shape[1]
    tokens = ids.shape[1]
    expert = iota((experts, tokens), 0)
    named = (ids[0:1, :] == expert) | (ids[1:2, :] == expert)
    earlier = bits(iota((tokens, tokens), 0) < iota((tokens, tokens), 1))
    rank = dot(bits(named), earlier)
    own = iota((experts, experts), 0) == iota((experts, experts), 1)
    limit = jnp.sum(jnp.where(own, capacity.astype(F32), 0.0), axis=1, keepdims=True)
    return jnp.where(named & (rank < limit), rank, NONE)


def combine_weights(v_ref, ids, key, q):
    expert = iota(key.shape, 0)
    scale = q.astype(F32) / 65536.0
    weight = jnp.where(ids[0:1, :] == expert, scale[0:1, :], 0.0) + jnp.where(ids[1:2, :] == expert, scale[1:2, :], 0.0)
    key, weight = key.T, weight.T
    peers = key.shape[1]
    for s in range(SLOTS):
        v_ref[:, s * peers : (s + 1) * peers] = jnp.where(key == float(s), weight, 0.0).astype(BF16)


BLOCK = 256
ONCHIP = pl.BlockSpec(memory_space=pltpu.VMEM)
REMOTE = pl.BlockSpec(memory_space=pltpu.HBM)


def fetch(copies):
    for c in copies:
        c.start()
    return copies


def flat_scratch(rows):
    return pltpu.VMEM((LANES // 128, rows, 128), F32)


PARTS = 8


def pack_body(
    ids_hbm, cap_hbm, q_hbm, tok_hbm, w_hbm, out_ref, v_ref, ids_ref, cap_ref, q_ref, tok_ref, w_ref, acc_ref, pick_ref,
    flat_ref, sems,
):
    part = w_ref.shape[0] // PARTS
    small = [
        pltpu.make_async_copy(frm, to, sems.at[2 * PARTS + n])
        for n, (frm, to) in enumerate(((ids_hbm, ids_ref), (cap_hbm, cap_ref), (q_hbm, q_ref)))
    ]
    fetch(small)
    gets = []
    for n in range(PARTS):
        at = pl.ds(n * part, part)
        gets.append(pltpu.make_async_copy(tok_hbm.at[:, at], tok_ref.at[:, at], sems.at[2 * n]))
        gets.append(pltpu.make_async_copy(w_hbm.at[at, :], w_ref.at[at, :], sems.at[2 * n + 1]))
    fetch(gets)
    for get in small:
        get.wait()
    ids = ids_ref[...]
    peers = pick_ref.shape[0] // SLOTS
    key = slot_keys(ids, cap_ref[...])
    for s in range(SLOTS):
        pick_ref[s * peers : (s + 1) * peers, :] = bits(key == float(s))
    combine_weights(v_ref, ids, key, q_ref[...])
    for n in range(PARTS):
        gets[2 * n].wait()
        gets[2 * n + 1].wait()
        at = slice(n * part, (n + 1) * part)
        product = dot(tok_ref[:, at], w_ref[at, :])
        acc_ref[...] = product if n == 0 else acc_ref[...] + product
    to_flat(flat_ref, dot(pick_ref[...], acc_ref[...].astype(BF16)))
    from_flat(out_ref, flat_ref)


def split_and_pack(ids, capacity, q, tokens, w_split):
    count = tokens.shape[0]
    limits = capacity[None, :]
    experts = limits.shape[1]
    rows = experts * ROWS
    return pl.pallas_call(
        pack_body,
        in_specs=[REMOTE] * 5,
        out_specs=[ONCHIP] * 2,
        out_shape=[
            jax.ShapeDtypeStruct((rows, LANES), BF16),
            jax.ShapeDtypeStruct((count, experts * SLOTS), BF16),
        ],
        scratch_shapes=[
            pltpu.VMEM(ids.shape, I32),
            pltpu.VMEM(limits.shape, I32),
            pltpu.VMEM(q.shape, I32),
            pltpu.VMEM(tokens.shape, BF16),
            pltpu.VMEM(w_split.shape, BF16),
            pltpu.VMEM((count, w_split.shape[1]), F32),
            pltpu.VMEM((experts * SLOTS, count), BF16),
            flat_scratch(rows),
            pltpu.SemaphoreType.DMA((2 * PARTS + 3,)),
        ],
        compiler_params=pltpu.CompilerParams(vmem_limit_bytes=SPLIT << 10),
        name="split_pack",
    )(*[pltpu.with_memory_space_constraint(a, pltpu.HBM) for a in (ids, limits, q, tokens, w_split)])


def expert_body(x_ref, in_ref, down_ref, out_ref, rows_ref, act_ref, flat_ref):
    hidden, width = down_ref.shape[1:]
    from_tiles(rows_ref, flat_ref, x_ref)
    rows = rows_ref[...]
    for j in range(0, hidden, BLOCK):
        gate = dot(rows, in_ref[0, :, j : j + BLOCK])
        up = dot(rows, in_ref[0, :, hidden + j : hidden + j + BLOCK])
        act_ref[:, j : j + BLOCK] = (gate / (1.0 + jnp.exp(-gate)) * up).astype(BF16)
    for j in range(0, width, BLOCK):
        to_flat(flat_ref, dot(act_ref[...], down_ref[0, :, j : j + BLOCK]), j)
    from_flat(out_ref, flat_ref)


def expert_rows(tiles, expert_in, expert_out):
    rows = tiles.shape[0]
    slots = rows // ROWS * SLOTS
    width = expert_in.shape[1]
    hidden = expert_out.shape[1]
    return pl.pallas_call(
        expert_body,
        in_specs=[ONCHIP] * 3,
        out_specs=ONCHIP,
        out_shape=jax.ShapeDtypeStruct((rows, LANES), BF16),
        scratch_shapes=[pltpu.VMEM((slots, width), BF16), pltpu.VMEM((slots, hidden), BF16), flat_scratch(rows)],
        compiler_params=pltpu.CompilerParams(vmem_limit_bytes=EXPERTS << 20),
        name="experts",
    )(tiles, expert_in, expert_out)


FIRST = 256


def column_block(w_ref, other, half=None):
    width = w_ref.shape[0]
    start, size = {None: (0, width), 0: (0, FIRST), 1: (FIRST, width - FIRST)}[half]
    return w_ref[:, pl.ds(pl.multiple_of((lax.axis_index("sub") ^ other) * width + start, 128), size)]


MERGE = pltpu.CompilerParams(vmem_limit_bytes=MERGE_MIB << 20)


def combine_body(v_ref, b_ref, w_ref, head_ref, send_ref, keep_ref, flat_ref):
    peers = b_ref.shape[0] // ROWS
    for b in range(LANES // 128):
        flat_ref[b] = b_ref[:, b * 128 : (b + 1) * 128].astype(F32)
    head = jnp.zeros(head_ref.shape, F32)
    for first in range(0, SLOTS, 2):
        answers = []
        for s in (first, first + 1):
            parts = [
                flat_ref[(lane + w) // 128, pl.ds(row, peers, stride=ROWS), :].astype(BF16)
                for row, lane, col, width in pieces(s)
                for w in range(0, width, 128)
            ]
            answers.append(jnp.concatenate(parts, axis=1))
        head += dot(v_ref[:, first * peers : (first + 2) * peers], jnp.concatenate(answers, axis=0))
    head = head.astype(BF16)
    head_ref[...] = head
    send_ref[...] = dot(head, column_block(w_ref, 3, 0)).astype(BF16)
    keep_ref[...] = dot(head, column_block(w_ref, 2, 0)).astype(BF16)


def combine_and_merge(v, back, w_merge):
    tokens = v.shape[0]
    width = w_merge.shape[0]
    rows = back.shape[0]
    return pl.pallas_call(
        combine_body,
        in_specs=[ONCHIP] * 3,
        out_specs=[ONCHIP] * 3,
        out_shape=[
            jax.ShapeDtypeStruct((tokens, width), BF16),
            jax.ShapeDtypeStruct((tokens, FIRST), BF16),
            jax.ShapeDtypeStruct((tokens, FIRST), BF16),
        ],
        scratch_shapes=[flat_scratch(rows)],
        compiler_params=MERGE,
        name="combine_merge",
    )(v, back, w_merge)


def far_body(blocks, head_ref, w_ref, *out_refs):
    for (other, half), out_ref in zip(blocks, out_refs):
        out_ref[...] = dot(head_ref[...], column_block(w_ref, other, half)).astype(BF16)


def merge_far(head, w_merge, blocks):
    tokens, width = head.shape
    return pl.pallas_call(
        functools.partial(far_body, blocks),
        in_specs=[ONCHIP] * 2,
        out_specs=[ONCHIP] * len(blocks),
        out_shape=[jax.ShapeDtypeStruct((tokens, (FIRST, width - FIRST)[half]), BF16) for _, half in blocks],
        compiler_params=MERGE,
    )(head, w_merge)


def own_body(head_ref, w_ref, after_ref, send_ref, keep_ref):
    del after_ref
    head = head_ref[...]
    send_ref[...] = dot(head, column_block(w_ref, 1)).astype(BF16)
    keep_ref[...] = dot(head, column_block(w_ref, 0)).astype(BF16)


def merge_own(head, w_merge, after):
    return pl.pallas_call(
        own_body,
        in_specs=[ONCHIP] * 2 + [REMOTE],
        out_specs=[ONCHIP] * 2,
        out_shape=[jax.ShapeDtypeStruct(head.shape, BF16)] * 2,
        compiler_params=MERGE,
        name="merge_own",
    )(head, w_merge, after)


WRITES = 4


def own_sum_body(keep_ref, in_ref, out_ref):
    out_ref[...] = keep_ref[...].astype(F32) + in_ref[...].astype(F32)


def own_sum(own_keep, own_in):
    return pl.pallas_call(
        own_sum_body,
        in_specs=[ONCHIP] * 2,
        out_specs=ONCHIP,
        out_shape=jax.ShapeDtypeStruct(own_keep.shape, F32),
        compiler_params=MERGE,
        name="own_sum",
    )(own_keep, own_in)


def last_body(own_ref, cross_0_ref, cross_1_ref, out_hbm, sum_ref, sems):
    rows = sum_ref.shape[0] // WRITES
    puts = []
    for n in range(WRITES):
        at = slice(n * rows, (n + 1) * rows)
        own = own_ref[at, :]
        sum_ref[at, :FIRST] = (own[:, :FIRST] + cross_0_ref[at, :].astype(F32)).astype(BF16)
        sum_ref[at, FIRST:] = (own[:, FIRST:] + cross_1_ref[at, :].astype(F32)).astype(BF16)
        piece = pl.ds(n * rows, rows)
        puts += fetch([pltpu.make_async_copy(sum_ref.at[piece, :], out_hbm.at[piece, :], sems.at[n])])
    for put in puts:
        put.wait()


def last_sum(own, cross_0, cross_1):
    return pl.pallas_call(
        last_body,
        in_specs=[ONCHIP] * 3,
        out_specs=REMOTE,
        out_shape=jax.ShapeDtypeStruct(own.shape, BF16),
        scratch_shapes=[pltpu.VMEM(own.shape, BF16), pltpu.SemaphoreType.DMA((WRITES,))],
        compiler_params=MERGE,
        name="last_sum",
    )(own, cross_0, cross_1)


def exchange(tiles, axes):
    peers = tiles.shape[0] // ROWS
    return lax.all_to_all(tiles.reshape(peers, ROWS, LANES), axes, split_axis=0, concat_axis=0, tiled=True).reshape(tiles.shape)


def added(a, b):
    return (a.astype(F32) + b.astype(F32)).astype(BF16)


def body(tokens, w_split, w_merge, expert_in, expert_out, expert_ids, combine_q, capacity):
    ids = expert_ids[0].T
    q = combine_q[0].T
    axes = ("seq", "sub")
    packed, v = split_and_pack(ids, capacity, q, tokens, w_split)
    tiles = exchange(packed, axes)
    back = exchange(expert_rows(tiles, expert_in, expert_out), axes)

    core = [(i, i ^ 1) for i in range(4)]
    chip = [(i, i ^ 2) for i in range(4)]
    head, send_0, keep_0 = combine_and_merge(v, back, w_merge)
    in_0 = lax.ppermute(send_0, "sub", core)
    (send_1,) = merge_far(head, w_merge, ((3, 1),))
    in_1 = lax.ppermute(send_1, "sub", core)
    (keep_1,) = merge_far(head, w_merge, ((2, 1),))
    far_0 = added(keep_0, in_0)
    cross_0 = lax.ppermute(far_0, "sub", chip)
    far_1 = added(keep_1, in_1)
    cross_1 = lax.ppermute(far_1, "sub", chip)
    own_send, own_keep = merge_own(head, w_merge, far_1)
    own_in = lax.ppermute(own_send, "sub", core)
    own = own_sum(own_keep, own_in)
    return last_sum(own, cross_0, cross_1)


def solution(mesh):
    in_specs = (
        P("seq", None),
        P(None, "sub"),
        P("sub", None),
        P(("seq", "sub"), None, None),
        P(("seq", "sub"), None, None),
        P("sub", "seq", None),
        P("sub", "seq", None),
        P(),
    )
    out_specs = P("seq", "sub")
    return jax.shard_map(body, mesh=mesh, in_specs=in_specs, out_specs=out_specs, check_vma=False)
```
